32 devices in a mesh: pair: 2 (over x), tp: 4 (over z), side: 4 (over y, core).
Axes of the slice: x: 2, y: 2, z: 4, core: 2. Of those that a mesh axis runs over, the one named last changes fastest.
Arguments:
- x_prompt: bfloat16 [8, 512, 7168], P(('pair', 'side')), parts along dimension 0
- s_len: int32 [8], P(('pair', 'side')), parts along dimension 0
- y_tok: bfloat16 [8, 4, 7168], P(('pair', 'side')), parts along dimension 0
- k_cache: bfloat16 [8, 1, 4, 64, 128, 192], P(('pair', 'side'), None, None, None, 'tp'), parts along dimension 0
- v_cache: bfloat16 [8, 1, 4, 64, 128, 128], P(('pair', 'side'), None, None, None, 'tp'), parts along dimension 0
- c_len: int32 [8, 4], P(('pair', 'side')), parts along dimension 0
- attn_gain: bfloat16 [1, 7168], replicated
- w_q: bfloat16 [1, 7168, 128, 192], P(None, None, 'tp')
- w_dkv: bfloat16 [1, 7168, 576], replicated
- w_uk: bfloat16 [1, 512, 128, 128], P(None, None, 'tp')
- w_uv: bfloat16 [1, 512, 128, 128], P(None, None, 'tp')
- w_o: bfloat16 [1, 128, 128, 7168], P(None, 'tp')
- mlp_gain: bfloat16 [1, 7168], replicated
- w_gate: bfloat16 [1, 7168, 2048], P(None, None, 'tp')
- w_up: bfloat16 [1, 7168, 2048], P(None, None, 'tp')
- w_down: bfloat16 [1, 2048, 7168], P(None, 'tp')
Outputs:
- output 1: bfloat16 [8, 512, 7168], P(('pair', 'side')), parts along dimension 0
- output 2: bfloat16 [8, 4, 7168], P(('pair', 'side')), parts along dimension 0
- output 3: bfloat16 [8, 1, 512, 128, 192], P(('pair', 'side'), None, None, 'tp'), parts along dimension 0
- output 4: bfloat16 [8, 1, 512, 128, 128], P(('pair', 'side'), None, None, 'tp'), parts along dimension 0
- output 5: bfloat16 [8, 1, 4, 64, 128, 192], P(('pair', 'side'), None, None, None, 'tp'), parts along dimension 0
- output 6: bfloat16 [8, 1, 4, 64, 128, 128], P(('pair', 'side'), None, None, None, 'tp'), parts along dimension 0
There are 2 independent parts. The reference program is written for one: setup_inputs(seed, part) draws one part's arguments, and reference() takes and returns one part's arrays. A program takes and returns all parts, laid end to end along the dimension named above; an argument that names none is the same for every part.
All inputs are finite; a program needn't handle non-finite values.
Results may differ from the reference program's by a relative error of at most 0.0109002.
Values are sent between devices in bfloat16 or wider.
A program may use at most 1 GiB of HBM per device.

```python
import math
import jax
import jax.numpy as jnp
from jax import lax

GROUPS = 4
PROMPT = 512
BATCH = 4
CACHE = 64
LAYERS = 1
DMODEL = 7168
HEADS = 128
NOPE = 128
ROPE_DIM = 64
VDIM = 128
KV_RANK = 512
FFN = 2048
QK_DIM = NOPE + ROPE_DIM
SCALE_QK = QK_DIM ** -0.5
Q_SCALE = (math.log(PROMPT) / 2.0) ** 0.5
EPSILON = 1e-6
THETA = 10000.0


def normal_bf16(key_in, dim_list, scale_val):
    return (jax.random.normal(key_in, dim_list, jnp.float32) * scale_val).astype(jnp.bfloat16)


def setup_inputs(seed: int = 0, part: int = 0) -> dict:
    part_keys = jax.random.split(jax.random.fold_in(jax.random.key(seed), part), 6)
    shared_keys = jax.random.split(jax.random.key(seed + 1), 10)
    s_len = jax.random.randint(part_keys[1], (GROUPS,), PROMPT // 2, PROMPT + 1).at[0].set(PROMPT)
    c_len = jax.random.randint(part_keys[5], (GROUPS, BATCH), CACHE // 2, CACHE).at[:, 0].set(CACHE - 1)
    return {
        'x_prompt': normal_bf16(part_keys[0], (GROUPS, PROMPT, DMODEL), 1.0),
        's_len': s_len,
        'y_tok': normal_bf16(part_keys[2], (GROUPS, BATCH, DMODEL), 1.0),
        'k_cache': normal_bf16(part_keys[3], (GROUPS, LAYERS, BATCH, CACHE, HEADS, QK_DIM), 1.0),
        'v_cache': normal_bf16(part_keys[4], (GROUPS, LAYERS, BATCH, CACHE, HEADS, VDIM), 1.0),
        'c_len': c_len,
        'attn_gain': jax.random.uniform(shared_keys[0], (LAYERS, DMODEL), jnp.float32, 0.5, 1.5).astype(jnp.bfloat16),
        'w_q': normal_bf16(shared_keys[1], (LAYERS, DMODEL, HEADS, QK_DIM), Q_SCALE * DMODEL ** -0.5),
        'w_dkv': normal_bf16(shared_keys[2], (LAYERS, DMODEL, KV_RANK + ROPE_DIM), DMODEL ** -0.5),
        'w_uk': normal_bf16(shared_keys[3], (LAYERS, KV_RANK, HEADS, NOPE), KV_RANK ** -0.5),
        'w_uv': normal_bf16(shared_keys[4], (LAYERS, KV_RANK, HEADS, VDIM), KV_RANK ** -0.5),
        'w_o': normal_bf16(shared_keys[5], (LAYERS, HEADS, VDIM, DMODEL), 2.0 * (HEADS * VDIM) ** -0.5),
        'mlp_gain': jax.random.uniform(shared_keys[6], (LAYERS, DMODEL), jnp.float32, 0.5, 1.5).astype(jnp.bfloat16),
        'w_gate': normal_bf16(shared_keys[7], (LAYERS, DMODEL, FFN), DMODEL ** -0.5),
        'w_up': normal_bf16(shared_keys[8], (LAYERS, DMODEL, FFN), DMODEL ** -0.5),
        'w_down': normal_bf16(shared_keys[9], (LAYERS, FFN, DMODEL), FFN ** -0.5),
    }


def mixed_einsum(form, left, right):
    return jnp.einsum(form, left.astype(jnp.float32), right.astype(jnp.float32))


def rms_scaled(values, gain):
    hidden = values.astype(jnp.float32)
    inv_rms = lax.rsqrt(jnp.mean(hidden * hidden, axis=-1, keepdims=True) + EPSILON)
    return (hidden * inv_rms * gain.astype(jnp.float32)).astype(jnp.bfloat16)


def rms_plain(values):
    hidden = values.astype(jnp.float32)
    inv_rms = lax.rsqrt(jnp.mean(hidden * hidden, axis=-1, keepdims=True) + EPSILON)
    return (hidden * inv_rms).astype(jnp.bfloat16)


def apply_rope(values, positions):
    half_dim = values.shape[-1] // 2
    inv_freq = THETA ** (-jnp.arange(half_dim, dtype=jnp.float32) * 2.0 / values.shape[-1])
    angles = positions.astype(jnp.float32)[..., None] * inv_freq
    cos_part = jnp.cos(angles)
    sin_part = jnp.sin(angles)
    first_half = values[..., :half_dim].astype(jnp.float32)
    second_half = values[..., half_dim:].astype(jnp.float32)
    return jnp.concatenate([first_half * cos_part - second_half * sin_part, second_half * cos_part + first_half * sin_part], axis=-1).astype(jnp.bfloat16)


def mlp_block(normed, w_gate_l, w_up_l, w_down_l):
    gate_val = jnp.dot(normed, w_gate_l, preferred_element_type=jnp.float32)
    up_val = jnp.dot(normed, w_up_l, preferred_element_type=jnp.float32)
    act_val = (jax.nn.silu(gate_val) * up_val).astype(jnp.bfloat16)
    return jnp.dot(act_val, w_down_l, preferred_element_type=jnp.float32).astype(jnp.bfloat16)


def prefill_group(x_one, len_one, weights):
    positions = jnp.arange(PROMPT)
    allowed = (positions[None, :] <= positions[:, None]) & (positions[None, :] < len_one)

    def head_attention(head_item):
        q_head, k_head, v_head = head_item
        scores = jnp.dot(q_head, k_head.T, preferred_element_type=jnp.float32) * SCALE_QK
        probs_bf = jax.nn.softmax(jnp.where(allowed, scores, -1e30), axis=-1).astype(jnp.bfloat16)
        return jnp.dot(probs_bf, v_head, preferred_element_type=jnp.float32).astype(jnp.bfloat16)

    def layer_step(hidden, layer_w):
        gain_attn, w_q_l, w_dkv_l, w_uk_l, w_uv_l, w_o_l, gain_mlp, w_gate_l, w_up_l, w_down_l = layer_w
        normed = rms_scaled(hidden, gain_attn)
        query_all = mixed_einsum('sd,dhe->she', normed, w_q_l).astype(jnp.bfloat16)
        query_all = jnp.concatenate([query_all[:, :, :NOPE], apply_rope(query_all[:, :, NOPE:], positions[:, None])], axis=-1)
        latent_raw = jnp.dot(normed, w_dkv_l, preferred_element_type=jnp.float32).astype(jnp.bfloat16)
        latent = rms_plain(latent_raw[:, :KV_RANK])
        rope_key = apply_rope(latent_raw[:, KV_RANK:], positions)
        key_nope = mixed_einsum('sr,rhn->shn', latent, w_uk_l).astype(jnp.bfloat16)
        value_full = mixed_einsum('sr,rhv->shv', latent, w_uv_l).astype(jnp.bfloat16)
        key_full = jnp.concatenate([key_nope, jnp.broadcast_to(rope_key[:, None, :], (PROMPT, HEADS, ROPE_DIM))], axis=-1)
        attn_heads = lax.map(head_attention, (jnp.transpose(query_all, (1, 0, 2)), jnp.transpose(key_full, (1, 0, 2)), jnp.transpose(value_full, (1, 0, 2))))
        hidden = hidden + mixed_einsum('hsv,hvd->sd', attn_heads, w_o_l).astype(jnp.bfloat16)
        hidden = hidden + mlp_block(rms_scaled(hidden, gain_mlp), w_gate_l, w_up_l, w_down_l)
        return hidden, (key_full, value_full)

    hidden_out, cache_pair = lax.scan(layer_step, x_one, weights)
    return hidden_out, cache_pair[0], cache_pair[1]


def decode_group(y_one, k_one, v_one, len_vec, weights):
    slot_hit = (jnp.arange(CACHE)[None, :] == len_vec[:, None])[:, :, None, None]
    allowed = jnp.arange(CACHE)[None, None, :] <= len_vec[:, None, None]

    def layer_step(tok_state, layer_in):
        layer_w, key_old, value_old = layer_in
        gain_attn, w_q_l, w_dkv_l, w_uk_l, w_uv_l, w_o_l, gain_mlp, w_gate_l, w_up_l, w_down_l = layer_w
        normed = rms_scaled(tok_state, gain_attn)
        query_all = mixed_einsum('bd,dhe->bhe', normed, w_q_l).astype(jnp.bfloat16)
        query_all = jnp.concatenate([query_all[:, :, :NOPE], apply_rope(query_all[:, :, NOPE:], len_vec[:, None])], axis=-1)
        latent_raw = jnp.dot(normed, w_dkv_l, preferred_element_type=jnp.float32).astype(jnp.bfloat16)
        latent = rms_plain(latent_raw[:, :KV_RANK])
        rope_key = apply_rope(latent_raw[:, KV_RANK:], len_vec)
        key_nope = mixed_einsum('br,rhn->bhn', latent, w_uk_l).astype(jnp.bfloat16)
        value_new = mixed_einsum('br,rhv->bhv', latent, w_uv_l).astype(jnp.bfloat16)
        key_new = jnp.concatenate([key_nope, jnp.broadcast_to(rope_key[:, None, :], (BATCH, HEADS, ROPE_DIM))], axis=-1)
        key_layer = jnp.where(slot_hit, key_new[:, None], key_old)
        value_layer = jnp.where(slot_hit, value_new[:, None], value_old)
        scores = mixed_einsum('bhe,bthe->bht', query_all, key_layer) * SCALE_QK
        probs_bf = jax.nn.softmax(jnp.where(allowed, scores, -1e30), axis=-1).astype(jnp.bfloat16)
        attn_val = mixed_einsum('bht,bthv->bhv', probs_bf, value_layer).astype(jnp.bfloat16)
        tok_state = tok_state + mixed_einsum('bhv,hvd->bd', attn_val, w_o_l).astype(jnp.bfloat16)
        tok_state = tok_state + mlp_block(rms_scaled(tok_state, gain_mlp), w_gate_l, w_up_l, w_down_l)
        return tok_state, (key_layer, value_layer)

    tok_out, cache_pair = lax.scan(layer_step, y_one, (weights, k_one, v_one))
    return tok_out, cache_pair[0], cache_pair[1]


def reference(x_prompt, s_len, y_tok, k_cache, v_cache, c_len, attn_gain, w_q, w_dkv, w_uk, w_uv, w_o, mlp_gain, w_gate, w_up, w_down):
    weights = (attn_gain, w_q, w_dkv, w_uk, w_uv, w_o, mlp_gain, w_gate, w_up, w_down)

    def prefill_one(group_item):
        return prefill_group(group_item[0], group_item[1], weights)

    def decode_one(group_item):
        return decode_group(group_item[0], group_item[1], group_item[2], group_item[3], weights)

    hidden_out, key_all, value_all = lax.map(prefill_one, (x_prompt, s_len))
    tok_out, key_next, value_next = lax.map(decode_one, (y_tok, k_cache, v_cache, c_len))
    return (hidden_out, tok_out, jnp.roll(key_all, 1, axis=0), jnp.roll(value_all, 1, axis=0), key_next, value_next)
```

```python
import functools
import jax
import jax.numpy as jnp
from jax import lax
from jax.experimental import pallas as pl
from jax.experimental.pallas import tpu as pltpu
from jax.sharding import PartitionSpec as P

EPSILON = 1e-6
THETA = 10000.0
TOK_PAD = 8
END_LAG = 6
MID_LAG = 2


def rms_scaled(values, gain):
    hidden = values.astype(jnp.float32)
    inv_rms = lax.rsqrt(jnp.mean(hidden * hidden, axis=-1, keepdims=True) + EPSILON)
    return (hidden * inv_rms * gain.astype(jnp.float32)).astype(jnp.bfloat16)


def rms_plain(values):
    hidden = values.astype(jnp.float32)
    inv_rms = lax.rsqrt(jnp.mean(hidden * hidden, axis=-1, keepdims=True) + EPSILON)
    return (hidden * inv_rms).astype(jnp.bfloat16)


def apply_rope(values, positions):
    half_dim = values.shape[-1] // 2
    inv_freq = THETA ** (-jnp.arange(half_dim, dtype=jnp.float32) * 2.0 / values.shape[-1])
    angles = positions.astype(jnp.float32)[..., None] * inv_freq
    cos_part = jnp.cos(angles)
    sin_part = jnp.sin(angles)
    first_half = values[..., :half_dim].astype(jnp.float32)
    second_half = values[..., half_dim:].astype(jnp.float32)
    return jnp.concatenate([first_half * cos_part - second_half * sin_part, second_half * cos_part + first_half * sin_part], axis=-1).astype(jnp.bfloat16)


def rope_query(query_all, positions, nope_dim):
    return jnp.concatenate([query_all[..., :nope_dim], apply_rope(query_all[..., nope_dim:], positions[:, None])], axis=-1)


def make_latent(normed, w_dkv_layer, positions, rank_dim):
    latent_raw = jnp.dot(normed, w_dkv_layer, preferred_element_type=jnp.float32).astype(jnp.bfloat16)
    return jnp.concatenate([rms_plain(latent_raw[:, :rank_dim]), apply_rope(latent_raw[:, rank_dim:], positions)], axis=-1)


def expand_latent(latent_pack, w_uk_layer, w_uv_layer):
    rank_dim = w_uk_layer.shape[0]
    latent = latent_pack[:, :rank_dim]
    rope_key = latent_pack[:, rank_dim:]
    key_nope = jnp.einsum('sr,rhn->shn', latent, w_uk_layer, preferred_element_type=jnp.float32).astype(jnp.bfloat16)
    value_full = jnp.einsum('sr,rhv->shv', latent, w_uv_layer, preferred_element_type=jnp.float32).astype(jnp.bfloat16)
    rope_heads = jnp.broadcast_to(rope_key[:, None, :], (key_nope.shape[0], key_nope.shape[1], rope_key.shape[1]))
    return jnp.concatenate([key_nope, rope_heads], axis=-1), value_full


def masked_softmax(scores, allowed):
    return jax.nn.softmax(jnp.where(allowed, scores, -1e30), axis=-1).astype(jnp.bfloat16)


def prompt_probs(query_all, key_full, valid_len):
    seq_len = query_all.shape[0]
    scores = jnp.einsum('qhe,khe->hqk', query_all, key_full, preferred_element_type=jnp.float32) * query_all.shape[-1] ** -0.5
    row_pos = jnp.arange(seq_len)[:, None]
    col_pos = jnp.arange(seq_len)[None, :]
    allowed = (col_pos <= row_pos) & (col_pos < valid_len)
    return masked_softmax(scores, allowed[None])


def cache_attention(query_all, key_layer, value_layer, cur_len):
    scores = jnp.einsum('bhe,bthe->bht', query_all, key_layer, preferred_element_type=jnp.float32) * query_all.shape[-1] ** -0.5
    allowed = jnp.arange(key_layer.shape[1])[None, None, :] <= cur_len[:, None, None]
    probs_bf = masked_softmax(scores, allowed)
    return jnp.einsum('bht,bthv->bhv', probs_bf, value_layer, preferred_element_type=jnp.float32).astype(jnp.bfloat16)


def line_barrier(zi, zn, more=0):
    sem = pltpu.get_barrier_semaphore()

    if more:
        side = lax.axis_index('side')
        pl.semaphore_signal(sem, inc=1, device_id={'side': side + 1 - 2 * lax.rem(side, 2)}, device_id_type=pl.DeviceIdType.MESH)

    @pl.when(zi > 0)
    def _():
        pl.semaphore_signal(sem, inc=1, device_id={'tp': zi - 1}, device_id_type=pl.DeviceIdType.MESH)

    @pl.when(zi < zn - 1)
    def _():
        pl.semaphore_signal(sem, inc=1, device_id={'tp': zi + 1}, device_id_type=pl.DeviceIdType.MESH)

    @pl.when((zi == 0) | (zi == zn - 1))
    def _():
        pl.semaphore_wait(sem, 1 + more)

    @pl.when((zi > 0) & (zi < zn - 1))
    def _():
        pl.semaphore_wait(sem, 2 + more)


def reduce_body(zn, nt, tn, hr, a_ref, x_ref, t_ref, w_ref, o_ref, ot_ref, wbuf, pdn, pup, rdn, rup, wsem, sdn, sup, vdn, vup):
    zi = lax.axis_index('tp')
    td = hr + TOK_PAD

    def wcopy(j):
        return pltpu.make_async_copy(w_ref.at[:, pl.ds(pl.multiple_of(j * tn, 128), tn)], wbuf.at[lax.rem(j, 2)], wsem.at[lax.rem(j, 2)])

    def send_dn(i):
        return pltpu.make_async_remote_copy(pdn.at[i], rdn.at[i], sdn.at[i], vdn.at[i], device_id={'tp': zi - 1}, device_id_type=pl.DeviceIdType.MESH)

    def send_up(i):
        return pltpu.make_async_remote_copy(pup.at[i], rup.at[i], sup.at[i], vup.at[i], device_id={'tp': zi + 1}, device_id_type=pl.DeviceIdType.MESH)

    lag = jnp.where((zi == 0) | (zi == zn - 1), END_LAG, MID_LAG)
    wcopy(0).start()
    line_barrier(zi, zn)

    def take_dn(i):
        @pl.when(zi < zn - 1)
        def _():
            send_dn(i).wait_recv()
            pdn[i] = pdn[i] + rdn[i]

            @pl.when(zi > 0)
            def _():
                send_dn(i).start()

        @pl.when(zi == 0)
        def _():
            cols = pl.ds(pl.multiple_of(i * tn, 128), tn)
            total = pdn[i]
            o_ref[:, cols] = x_ref[:, cols] + total[:hr].astype(jnp.bfloat16)
            ot_ref[:, cols] = (t_ref[:, cols].astype(jnp.bfloat16) + total[hr:].astype(jnp.bfloat16)).astype(jnp.float32)

    def take_up(i):
        @pl.when(zi > 0)
        def _():
            send_up(i).wait_recv()
            pup[i] = pup[i] + rup[i]

            @pl.when(zi < zn - 1)
            def _():
                send_up(i).start()

            cols = pl.ds(pl.multiple_of(i * tn, 128), tn)
            o_ref[:, cols] = x_ref[:, cols] + pup[i].astype(jnp.bfloat16)
            ot_ref[:, cols] = t_ref[:, cols]

    def handle(i):
        def ordered(near, far):
            @pl.when(i < nt)
            def _():
                near(i)

            @pl.when(i > 0)
            def _():
                far(i - 1)

        @pl.when(zi < zn // 2)
        def _():
            ordered(take_up, take_dn)

        @pl.when(zi >= zn // 2)
        def _():
            ordered(take_dn, take_up)

    @pl.loop(0, nt)
    def _(j):
        wcopy(j).wait()

        @pl.when(j + 1 < nt)
        def _():
            wcopy(j + 1).start()

        wt = wbuf[lax.rem(j, 2)]
        pdn[j] = jnp.dot(a_ref[:td], wt, preferred_element_type=jnp.float32)

        @pl.when(zi == zn - 1)
        def _():
            send_dn(j).start()

        pup[j] = jnp.dot(a_ref[td:], wt, preferred_element_type=jnp.float32)[:hr]

        @pl.when(zi == 0)
        def _():
            send_up(j).start()

        @pl.when(j >= lag)
        def _():
            handle(j - lag)

    @pl.loop(nt - lag, nt + 1)
    def _(j):
        handle(j)

    @pl.loop(0, nt)
    def _(j):
        @pl.when(zi > 0)
        def _():
            send_dn(j).wait_send()

        @pl.when(zi < zn - 1)
        def _():
            send_up(j).wait_send()


def reduce_call(a_rows, x_own, t_own, w_o, zn):
    hr, width = x_own.shape
    depth = a_rows.shape[1]
    tn = 256
    nt = width // tn
    td = hr + TOK_PAD
    vm = pl.BlockSpec(memory_space=pltpu.VMEM)
    return pl.pallas_call(
        functools.partial(reduce_body, zn, nt, tn, hr),
        out_shape=(jax.ShapeDtypeStruct((hr, width), jnp.bfloat16), jax.ShapeDtypeStruct((TOK_PAD, width), jnp.float32)),
        in_specs=[vm, vm, vm, pl.BlockSpec(memory_space=pl.ANY)],
        out_specs=(vm, vm),
        scratch_shapes=[
            pltpu.VMEM((2, depth, tn), jnp.bfloat16),
            pltpu.VMEM((nt, td, tn), jnp.float32),
            pltpu.VMEM((nt, hr, tn), jnp.float32),
            pltpu.VMEM((nt, td, tn), jnp.float32),
            pltpu.VMEM((nt, hr, tn), jnp.float32),
            pltpu.SemaphoreType.DMA((2,)),
            pltpu.SemaphoreType.DMA((nt,)),
            pltpu.SemaphoreType.DMA((nt,)),
            pltpu.SemaphoreType.DMA((nt,)),
            pltpu.SemaphoreType.DMA((nt,)),
        ],
        compiler_params=pltpu.CompilerParams(collective_id=0, has_side_effects=True, vmem_limit_bytes=66_000_000),
        cost_estimate=pl.CostEstimate(flops=2 * a_rows.shape[0] * depth * width, bytes_accessed=depth * width * 2, transcendentals=0),
        name='wo_reduce',
    )(a_rows, x_own, t_own, w_o)


def mlp_body(zn, nq, hr, fw, cw, *refs):
    b_ref, h_ref, t_ref, wg_ref, wu_ref, wd_ref = refs[:6]
    half = nq // 2
    n_in = 2 * nq
    pieces = refs[6:6 + n_in]
    o_ref, ot_ref, xc_ref, gacc, uacc, m_ref, wbuf, obuf, dbuf, wsem, dsem, xs, xr, sa, ra, sb, rb, st, rt = refs[6 + n_in:]
    zi = lax.axis_index('tp')
    side = lax.axis_index('side')
    qi = lax.axis_index('pair') * (nq // 2) + side
    slots = 4
    steps = slots * nq
    depth = 4

    def flip(e):
        out = 0
        for bit in (1, 2, 4):
            out = out + bit * lax.rem(lax.rem(qi // bit, 2) + lax.rem(e // bit, 2), 2)
        return out

    def cols_at(q):
        return pl.ds(pl.multiple_of(q * cw, 128), cw)

    order = [(s, e) for s in (0, 1) for e in range(nq)]
    order += [(s, e) for par in (0, 1) for s in (2, 3) for e in range(par, nq, 2)]

    def slot_piece(i):
        late = i - 2 * nq
        early = i < 2 * nq
        s = jnp.where(early, i // nq, 2 + lax.rem(late // half, 2))
        e = jnp.where(early, lax.rem(i, nq), 2 * lax.rem(late, half) + late // (2 * half))
        return s, e

    def cross(k, j):
        return pltpu.make_async_remote_copy(
            pieces[nq + k * half + j], xc_ref.at[k, j], xs.at[k, j], xr.at[k, j],
            device_id={'side': side + 1 - 2 * lax.rem(side, 2)}, device_id_type=pl.DeviceIdType.MESH)

    def source(s, e):
        if s == 1:
            return pieces[e]
        if e % 2 == 0:
            return pieces[nq + (s - 2) * half + e // 2]
        return xc_ref.at[s - 2, e // 2]

    line_barrier(zi, zn, 1)
    ends = (zi == 0) | (zi == zn - 1)

    def start_gu(i):
        buf = lax.rem(i, depth)

        @pl.when(i < nq)
        def _():
            rows = cols_at(flip(i))
            pltpu.make_async_copy(wg_ref.at[rows, :], wbuf.at[buf, 0], wsem.at[buf]).start()
            pltpu.make_async_copy(wu_ref.at[rows, :], wbuf.at[buf, 1], wsem.at[buf]).start()

        for k, (s, e) in enumerate(order):
            if s > 0:
                @pl.when(i == k)
                def _(s=s, e=e):
                    if s > 1 and e % 2:
                        cross(s - 2, e // 2).wait_recv()
                    pltpu.make_async_copy(source(s, e).at[pl.ds(0, 2)], wbuf.at[buf], wsem.at[buf]).start()

    def start_dn(e):
        pltpu.make_async_copy(wd_ref.at[:, cols_at(flip(e))], obuf.at[lax.rem(e, 2)], dsem.at[lax.rem(e, 2), 0]).start()
        for k in range(nq):
            @pl.when(e == k)
            def _(k=k):
                for s in range(1, slots):
                    pltpu.make_async_copy(source(s, k).at[2], dbuf.at[lax.rem(e, 2), s - 1], dsem.at[lax.rem(e, 2), s]).start()

    hh = hr // 2

    def block(h, r, q):
        return o_ref.at[pl.ds(h * hr + r * hh, hh), cols_at(q)]

    def up(q, r):
        return pltpu.make_async_remote_copy(block(0, r, q), block(0, r, q), sa.at[r, q], ra.at[r, q], device_id={'tp': zi + 1}, device_id_type=pl.DeviceIdType.MESH)

    def down(q, r):
        return pltpu.make_async_remote_copy(block(1, r, q), block(1, r, q), sb.at[r, q], rb.at[r, q], device_id={'tp': zi - 1}, device_id_type=pl.DeviceIdType.MESH)

    def tok(q):
        tile = ot_ref.at[:, cols_at(q)]
        return pltpu.make_async_remote_copy(tile, tile, st.at[q], rt.at[q], device_id={'tp': zi + 1}, device_id_type=pl.DeviceIdType.MESH)

    @pl.when(ends)
    def _():
        for k in range(2):
            for j in range(half):
                cross(k, j).start()
        for i in range(depth - 1):
            start_gu(jnp.int32(i))
        gacc[...] = jnp.zeros_like(gacc)
        uacc[...] = jnp.zeros_like(uacc)

        @pl.loop(0, steps)
        def _(i):
            buf = lax.rem(i, depth)
            s, e = slot_piece(i)
            pltpu.make_async_copy(pieces[0].at[pl.ds(0, 2)], wbuf.at[buf], wsem.at[buf]).wait()

            @pl.when(i + depth - 1 < steps)
            def _():
                start_gu(i + depth - 1)

            rows = b_ref[:, cols_at(flip(e))]
            gacc[s] = gacc[s] + jnp.dot(rows, wbuf[buf, 0], preferred_element_type=jnp.float32)
            uacc[s] = uacc[s] + jnp.dot(rows, wbuf[buf, 1], preferred_element_type=jnp.float32)

        start_dn(jnp.int32(0))

        @pl.loop(0, slots)
        def _(s):
            gate = gacc[s]
            m_ref[s] = (gate * jax.nn.sigmoid(gate) * uacc[s]).astype(jnp.bfloat16)

        @pl.loop(0, nq)
        def _(e):
            par = lax.rem(e, 2)
            q = flip(e)
            cols = cols_at(q)

            @pl.when(e + 1 < nq)
            def _():
                start_dn(e + 1)

            acc = None
            for s in range(slots):
                pltpu.make_async_copy(pieces[0].at[2], dbuf.at[par, max(s - 1, 0)], dsem.at[par, s]).wait()
                if s == 0:
                    acc = jnp.dot(m_ref[s], obuf[par], preferred_element_type=jnp.float32)
                else:
                    acc = acc + lax.dot_general(m_ref[s], dbuf[par, s - 1], (((1,), (1,)), ((), ())), preferred_element_type=jnp.float32)
            res = h_ref[:, cols] + acc[:hr].astype(jnp.bfloat16)

            @pl.when(zi == 0)
            def _():
                o_ref[:hr, cols] = res
                ot_ref[:, cols] = (t_ref[:, cols].astype(jnp.bfloat16) + acc[hr:hr + TOK_PAD].astype(jnp.bfloat16)).astype(jnp.float32)
                up(q, 0).start()
                up(q, 1).start()
                tok(q).start()

            @pl.when(zi == zn - 1)
            def _():
                o_ref[hr:, cols] = res
                down(q, 0).start()
                down(q, 1).start()

        for k in range(2):
            for j in range(half):
                cross(k, j).wait_send()

    @pl.when((zi > 0) & (zi < zn - 1))
    def _():
        @pl.loop(0, 2 * nq + 1)
        def _(i):
            def pass_up(n):
                q = flip(n // 2)
                up(q, lax.rem(n, 2)).wait_recv()
                up(q, lax.rem(n, 2)).start()

                @pl.when(lax.rem(n, 2) == 1)
                def _():
                    tok(q).wait_recv()
                    tok(q).start()

            def pass_down(n):
                q = flip(n // 2)
                down(q, lax.rem(n, 2)).wait_recv()
                down(q, lax.rem(n, 2)).start()

            def ordered(near, far):
                @pl.when(i < 2 * nq)
                def _():
                    near(i)

                @pl.when(i > 0)
                def _():
                    far(i - 1)

            @pl.when(zi < zn // 2)
            def _():
                ordered(pass_up, pass_down)

            @pl.when(zi >= zn // 2)
            def _():
                ordered(pass_down, pass_up)

    @pl.loop(0, nq)
    def _(q):
        @pl.when(zi == zn - 1)
        def _():
            up(q, 0).wait_recv()
            up(q, 1).wait_recv()
            tok(q).wait_recv()

        @pl.when(zi == 0)
        def _():
            down(q, 0).wait_recv()
            down(q, 1).wait_recv()

        @pl.when(zi < zn - 1)
        def _():
            up(q, 0).wait_send()
            up(q, 1).wait_send()
            tok(q).wait_send()

        @pl.when(zi > 0)
        def _():
            down(q, 0).wait_send()
            down(q, 1).wait_send()


def mlp_call(b_rows, h_rows, t_rows, w_gate, w_up, w_down, pieces, zn):
    hr, width = h_rows.shape
    br = b_rows.shape[0]
    nq = len(pieces) // 2
    fw = w_gate.shape[1]
    cw = width // nq
    vm = pl.BlockSpec(memory_space=pltpu.VMEM)
    hb = pl.BlockSpec(memory_space=pl.ANY)
    out = pl.pallas_call(
        functools.partial(mlp_body, zn, nq, hr, fw, cw),
        out_shape=(
            jax.ShapeDtypeStruct((2 * hr, width), jnp.bfloat16),
            jax.ShapeDtypeStruct((TOK_PAD, width), jnp.float32),
            jax.ShapeDtypeStruct((2, nq // 2, 3, cw, fw), jnp.bfloat16),
        ),
        in_specs=[vm, vm, vm] + [hb] * (3 + len(pieces)),
        out_specs=(vm, vm, hb),
        scratch_shapes=[
            pltpu.VMEM((4, br, fw), jnp.float32),
            pltpu.VMEM((4, br, fw), jnp.float32),
            pltpu.VMEM((4, br, fw), jnp.bfloat16),
            pltpu.VMEM((4, 2, cw, fw), jnp.bfloat16),
            pltpu.VMEM((2, fw, cw), jnp.bfloat16),
            pltpu.VMEM((2, 3, cw, fw), jnp.bfloat16),
            pltpu.SemaphoreType.DMA((4,)),
            pltpu.SemaphoreType.DMA((2, 4)),
            pltpu.SemaphoreType.DMA((2, nq // 2)),
            pltpu.SemaphoreType.DMA((2, nq // 2)),
        ] + [pltpu.SemaphoreType.DMA((2, nq)) for _ in range(4)] + [pltpu.SemaphoreType.DMA((nq,)) for _ in range(2)],
        compiler_params=pltpu.CompilerParams(collective_id=1, has_side_effects=True, vmem_limit_bytes=60_000_000),
        cost_estimate=pl.CostEstimate(flops=2 * br * 4 * fw * width * 3, bytes_accessed=4 * fw * width * 6, transcendentals=0),
        name='mlp_spread',
    )(b_rows, h_rows, t_rows, w_gate, w_up, w_down, *pieces)
    return out[0], out[1]


def own_piece(w_gate, w_up, w_down, nq):
    qi = lax.axis_index('pair') * (nq // 2) + lax.axis_index('side')
    cw = w_gate.shape[0] // nq
    return jnp.stack([
        lax.dynamic_slice_in_dim(w_gate, qi * cw, cw, 0),
        lax.dynamic_slice_in_dim(w_up, qi * cw, cw, 0),
        lax.dynamic_slice_in_dim(w_down, qi * cw, cw, 1).T,
    ])


def line_step(rise, fall, step, zn):
    rise = lax.ppermute(rise, 'tp', [(z, z + 1) for z in range(step - 1, zn - 1)])
    fall = lax.ppermute(fall, 'tp', [(z + 1, z) for z in range(0, zn - step)])
    return rise, fall


def plane_step(rise, fall, zn):
    mine = jnp.where(lax.axis_index('tp') < zn // 2, fall, rise)
    over_y = lax.ppermute(mine, 'side', [(0, 2), (2, 0), (1, 3), (3, 1)])
    over_x = lax.ppermute(mine, 'pair', [(0, 1), (1, 0)])
    over_d = lax.ppermute(mine, ('pair', 'side'), [(p * 4 + s, (1 - p) * 4 + (s + 2) % 4) for p in range(2) for s in range(4)])
    return [mine, over_y, over_x, over_d]


def core_step(parts):
    out = []
    for part in parts:
        out += [part, lax.ppermute(part, 'side', [(0, 1), (1, 0), (2, 3), (3, 2)])]
    return out


def tie(*values):
    return lax.optimization_barrier(values)


def solution(mesh):
    groups = mesh.shape['side']
    zn = mesh.shape['tp']
    nq = mesh.shape['pair'] * groups
    shift_pairs = [(source_idx, (source_idx + 1) % groups) for source_idx in range(groups)]
    group_axes = ('pair', 'side')
    head_spec = P(None, None, 'tp', None)
    cache_spec = P(group_axes, None, None, None, 'tp', None)
    prompt_spec = P(group_axes, None, None, 'tp', None)
    row_spec = P(group_axes, None, None)
    spec_in = (row_spec, P(group_axes), row_spec, cache_spec, cache_spec, P(group_axes, None), P(), head_spec, P(), head_spec, head_spec, P(None, 'tp', None, None), P(), P(None, None, 'tp'), P(None, None, 'tp'), P(None, 'tp', None))
    spec_out = (row_spec, row_spec, prompt_spec, prompt_spec, cache_spec, cache_spec)

    def device_step(x_prompt, s_len, y_tok, k_cache, v_cache, c_len, attn_gain, w_q, w_dkv, w_uk, w_uv, w_o, mlp_gain, w_gate, w_up, w_down):
        zi = lax.axis_index('tp')
        hidden, toks = x_prompt[0], y_tok[0]
        rows, width = hidden.shape
        nb = toks.shape[0]
        hr = rows // 2
        cur_len = c_len[0]
        own = own_piece(w_gate[0], w_up[0], w_down[0], nq)
        rise, fall = line_step(own, own, 1, zn)

        every = jnp.concatenate([hidden, toks, jnp.zeros((16 - nb, width), hidden.dtype)], axis=0)
        positions = jnp.concatenate([jnp.arange(rows, dtype=jnp.int32), cur_len, jnp.zeros((16 - nb,), jnp.int32)])
        normed = rms_scaled(every, attn_gain[0])
        latent_pack = make_latent(normed, w_dkv[0], positions, w_uk.shape[1])
        received = lax.ppermute(latent_pack[:rows], 'side', shift_pairs)
        query_raw = jnp.einsum('sd,dhe->she', normed, w_q[0], preferred_element_type=jnp.float32).astype(jnp.bfloat16)
        query_raw, rise, fall = tie(query_raw, rise, fall)
        first = plane_step(rise, fall, zn)
        rise, fall = line_step(rise, fall, 2, zn)
        query_all = rope_query(query_raw, positions, w_uk.shape[-1])
        key_all, value_all = expand_latent(latent_pack, w_uk[0], w_uv[0])
        probs = prompt_probs(query_all[:rows], key_all[:rows], s_len[0])
        probs, rise, fall = tie(probs, rise, fall)
        second = plane_step(rise, fall, zn)
        rise, fall = line_step(rise, fall, 3, zn)
        attn_val = jnp.einsum('hqk,khv->qhv', probs, value_all[:rows], preferred_element_type=jnp.float32).astype(jnp.bfloat16)

        key_new, value_new = key_all[rows:rows + nb], value_all[rows:rows + nb]
        key_old, value_old = k_cache[0, 0], v_cache[0, 0]
        slot_hit = (jnp.arange(key_old.shape[1])[None, :] == cur_len[:, None])[:, :, None, None]
        key_layer = jnp.where(slot_hit, key_new[:, None], key_old)
        value_layer = jnp.where(slot_hit, value_new[:, None], value_old)
        tok_val = cache_attention(query_all[rows:rows + nb], key_layer, value_layer, cur_len)

        heads = attn_val.shape[1] * attn_val.shape[2]
        attn_flat = attn_val.reshape(rows, heads)
        zpad = jnp.zeros((TOK_PAD - nb, heads), attn_flat.dtype)
        a_rows = jnp.concatenate([attn_flat[:hr], tok_val.reshape(nb, heads), zpad, attn_flat[hr:], jnp.zeros((TOK_PAD, heads), attn_flat.dtype)], axis=0)
        a_rows, rise, fall, first = tie(a_rows, rise, fall, first)
        third = plane_step(rise, fall, zn)
        first = core_step(first)
        x_own = lax.dynamic_slice_in_dim(hidden, jnp.where(zi < zn // 2, 0, hr), hr, 0)
        t_own = jnp.concatenate([toks, jnp.zeros((TOK_PAD - nb, width), toks.dtype)], axis=0).astype(jnp.float32)
        h_mid, t_mid = reduce_call(a_rows, x_own, t_own, w_o[0].reshape(heads, width), zn)

        key_in, value_in = expand_latent(received, w_uk[0], w_uv[0])

        b_rows = jnp.concatenate([
            rms_scaled(h_mid, mlp_gain[0]),
            rms_scaled(t_mid.astype(jnp.bfloat16), mlp_gain[0]),
            jnp.zeros((TOK_PAD, width), jnp.bfloat16),
        ], axis=0)
        h_out, t_out = mlp_call(b_rows, h_mid, t_mid, w_gate[0], w_up[0], w_down[0], first + second + third, zn)
        y_out = t_out[:nb].astype(jnp.bfloat16)
        return (h_out[None], y_out[None], key_in[None, None], value_in[None, None], key_layer[None, None], value_layer[None, None])

    return jax.shard_map(device_step, mesh=mesh, in_specs=spec_in, out_specs=spec_out, check_vma=False)
```

```python
import functools
import jax
import jax.numpy as jnp
from jax import lax
from jax.experimental import pallas as pl
from jax.experimental.pallas import tpu as pltpu
from jax.sharding import PartitionSpec as P

EPSILON = 1e-6
THETA = 10000.0
TOK_PAD = 8
dma = pltpu.SemaphoreType.DMA
mesh_id = pl.DeviceIdType.MESH
none = None
END_LAG = 6
RELAY_AT = (12, 21)
MID_LAG = 2


def rms_scaled(values, gain):
    hidden = values.astype(jnp.float32)
    inv_rms = lax.rsqrt(jnp.mean(hidden * hidden, axis=-1, keepdims=True) + EPSILON)
    return (hidden * inv_rms * gain.astype(jnp.float32)).astype(jnp.bfloat16)


def rms_plain(values):
    hidden = values.astype(jnp.float32)
    inv_rms = lax.rsqrt(jnp.mean(hidden * hidden, axis=-1, keepdims=True) + EPSILON)
    return (hidden * inv_rms).astype(jnp.bfloat16)


def apply_rope(values, positions):
    half_dim = values.shape[-1] // 2
    inv_freq = THETA ** (-jnp.arange(half_dim, dtype=jnp.float32) * 2.0 / values.shape[-1])
    angles = positions.astype(jnp.float32)[..., None] * inv_freq
    cos_part = jnp.cos(angles)
    sin_part = jnp.sin(angles)
    first_half = values[..., :half_dim].astype(jnp.float32)
    second_half = values[..., half_dim:].astype(jnp.float32)
    return jnp.concatenate([first_half * cos_part - second_half * sin_part, second_half * cos_part + first_half * sin_part], axis=-1).astype(jnp.bfloat16)


def rope_tables(positions, rope_dim):
    half_dim = rope_dim // 2
    inv_freq = THETA ** (-jnp.arange(half_dim, dtype=jnp.float32) * 2.0 / rope_dim)
    angles = positions.astype(jnp.float32)[..., None] * inv_freq
    return jnp.tile(jnp.cos(angles), (1, 4)), jnp.tile(jnp.sin(angles), (1, 4))


def make_latent(normed, w_dkv_layer, positions, rank_dim):
    latent_raw = jnp.dot(normed, w_dkv_layer, preferred_element_type=jnp.float32).astype(jnp.bfloat16)
    return jnp.concatenate([rms_plain(latent_raw[:, :rank_dim]), apply_rope(latent_raw[:, rank_dim:], positions)], axis=-1)


def expand_latent(latent_pack, w_uk_layer, w_uv_layer):
    rank_dim = w_uk_layer.shape[0]
    latent = latent_pack[:, :rank_dim]
    rope_key = latent_pack[:, rank_dim:]
    key_nope = jnp.einsum('sr,rhn->shn', latent, w_uk_layer, preferred_element_type=jnp.float32).astype(jnp.bfloat16)
    value_full = jnp.einsum('sr,rhv->shv', latent, w_uv_layer, preferred_element_type=jnp.float32).astype(jnp.bfloat16)
    rope_heads = jnp.broadcast_to(rope_key[:, None, :], (key_nope.shape[0], key_nope.shape[1], rope_key.shape[1]))
    return jnp.concatenate([key_nope, rope_heads], axis=-1), value_full


def masked_softmax(scores, allowed):
    return jax.nn.softmax(jnp.where(allowed, scores, -1e30), axis=-1).astype(jnp.bfloat16)


def cache_attention(query_all, key_layer, value_layer, cur_len):
    scores = jnp.einsum('bhe,bthe->bht', query_all, key_layer, preferred_element_type=jnp.float32) * query_all.shape[-1] ** -0.5
    allowed = jnp.arange(key_layer.shape[1])[None, None, :] <= cur_len[:, None, None]
    probs_bf = masked_softmax(scores, allowed)
    return jnp.einsum('bht,bthv->bhv', probs_bf, value_layer, preferred_element_type=jnp.float32).astype(jnp.bfloat16)


def line_barrier(zi, zn, also):
    sem = pltpu.get_barrier_semaphore()

    for one in also:
        pl.semaphore_signal(sem, inc=1, device_id=one, device_id_type=mesh_id)

    @pl.when(zi > 0)
    def _():
        pl.semaphore_signal(sem, inc=1, device_id={'tp': zi - 1}, device_id_type=mesh_id)

    @pl.when(zi < zn - 1)
    def _():
        pl.semaphore_signal(sem, inc=1, device_id={'tp': zi + 1}, device_id_type=mesh_id)

    @pl.when((zi == 0) | (zi == zn - 1))
    def _():
        pl.semaphore_wait(sem, 1 + len(also))

    @pl.when((zi > 0) & (zi < zn - 1))
    def _():
        pl.semaphore_wait(sem, 2 + len(also))


def attend_body(rows, nope, rope, scale, n_ref, w_ref, k_ref, r_ref, v_ref, cos_ref, sin_ref, len_ref, o_ref, qt_ref, acc):
    heads = w_ref.shape[0]
    depth = n_ref.shape[1]
    chunk = depth // 4
    lane = lax.broadcasted_iota(jnp.int32, (1, 2 * rope), 1)
    low = lane < rope
    first = lax.rem(lane, rope) < rope // 2
    wide = heads * (nope + rope)

    def part(c):
        span = pl.ds(pl.multiple_of(c * chunk, 128), chunk)
        return lax.dot_general(n_ref[:, span], w_ref[:, :, span].reshape(wide, chunk), (((1,), (1,)), ((), ())), preferred_element_type=jnp.float32)

    acc[...] = part(0)

    @pl.loop(1, 4)
    def _(c):
        acc[...] = acc[...] + part(c)

    cos, sin = cos_ref[...], sin_ref[...]
    valid = len_ref[0]
    kr = r_ref[...]
    half_rows = rows // 2
    for pair in range(heads // 2):
        base = pair * 2 * (nope + rope)
        t0, t1, t2 = (acc[:, base + nope * i:base + nope * (i + 1)].astype(jnp.bfloat16).astype(jnp.float32) for i in range(3))
        n1 = jnp.where(low, pltpu.roll(t1, rope, 1), pltpu.roll(t2, rope, 1))
        both = jnp.where(low, t1, t2)
        turned = jnp.where(first, -pltpu.roll(both, 2 * rope - rope // 2, 1), pltpu.roll(both, rope // 2, 1))
        both = both * cos + turned * sin
        for sub, nq in ((0, t0), (1, n1)):
            h = pair * 2 + sub
            keep = low if sub == 0 else jnp.logical_not(low)
            query = jnp.concatenate([nq.astype(jnp.bfloat16), jnp.where(keep, both, 0.0).astype(jnp.bfloat16)], axis=1)
            qt_ref[h] = query[rows:]
            for blk in range(2):
                span = (blk + 1) * half_rows
                key = jnp.concatenate([k_ref[h, :, :span], kr[:, :span]], axis=0)
                s = jnp.dot(query[blk * half_rows:(blk + 1) * half_rows], key, preferred_element_type=jnp.float32) * scale
                row = lax.broadcasted_iota(jnp.int32, s.shape, 0) + blk * half_rows
                col = lax.broadcasted_iota(jnp.int32, s.shape, 1)
                s = jnp.where((col <= row) & (col < valid), s, -1e30)
                p = jnp.exp(s - jnp.max(s, axis=1, keepdims=True))
                p = (p * (1.0 / jnp.sum(p, axis=1, keepdims=True))).astype(jnp.bfloat16)
                out = jnp.dot(p, v_ref[h, :span, :], preferred_element_type=jnp.float32)
                o_ref[blk * half_rows:(blk + 1) * half_rows, h * nope:(h + 1) * nope] = out.astype(jnp.bfloat16)


def attend_call(normed, w_q, key_t, rope_t, value, cos, sin, valid_len, rows, scale):
    total, depth = normed.shape
    heads, feat, _ = w_q.shape
    nope = key_t.shape[1]
    rope = feat - nope
    vdim = value.shape[2]
    grp = 4
    vm = pl.BlockSpec(memory_space=pltpu.VMEM)
    return pl.pallas_call(
        functools.partial(attend_body, rows, nope, rope, scale),
        grid=(heads // grp,),
        out_shape=(jax.ShapeDtypeStruct((rows, heads * vdim), jnp.bfloat16), jax.ShapeDtypeStruct((heads, total - rows, 2 * nope), jnp.bfloat16)),
        in_specs=[
            vm,
            pl.BlockSpec((grp, feat, depth), lambda g: (g, 0, 0)),
            pl.BlockSpec((grp, nope, key_t.shape[2]), lambda g: (g, 0, 0)),
            vm,
            pl.BlockSpec((grp, value.shape[1], vdim), lambda g: (g, 0, 0)),
            vm, vm,
            pl.BlockSpec(memory_space=pltpu.SMEM),
        ],
        out_specs=(pl.BlockSpec((rows, grp * vdim), lambda g: (0, g)), pl.BlockSpec((grp, total - rows, 2 * nope), lambda g: (g, 0, 0))),
        scratch_shapes=[pltpu.VMEM((total, grp * feat), jnp.float32)],
        compiler_params=pltpu.CompilerParams(vmem_limit_bytes=60_000_000),
        cost_estimate=pl.CostEstimate(flops=2 * total * depth * heads * feat + 3 * rows * rows * heads * feat, bytes_accessed=heads * feat * depth * 2, transcendentals=rows * rows * heads),
        name='attend',
    )(normed, w_q, key_t, rope_t, value, cos, sin, valid_len)


def reduce_body(zn, nt, tn, hr, p_ref, q_ref, x_ref, t_ref, w_ref, m2_ref, m3_ref, o_ref, ot_ref, g_ref, a_ref, asem, gs, gr, wbuf, pdn, pup, rdn, rup, wsem, sdn, sup, vdn, vup):
    zi = lax.axis_index('tp')

    def wcopy(j):
        return pltpu.make_async_copy(w_ref.at[:, pl.ds(pl.multiple_of(j * tn, 128), tn)], wbuf.at[lax.rem(j, 2)], wsem.at[lax.rem(j, 2)])

    def send_dn(i):
        return pltpu.make_async_remote_copy(pdn.at[i], rdn.at[i], sdn.at[i], vdn.at[i], device_id={'tp': zi - 1}, device_id_type=mesh_id)

    def send_up(i):
        return pltpu.make_async_remote_copy(pup.at[i], rup.at[i], sup.at[i], vup.at[i], device_id={'tp': zi + 1}, device_id_type=mesh_id)

    ends = (zi == 0) | (zi == zn - 1)
    lag = jnp.where(ends, END_LAG, MID_LAG)
    over_y = {'side': lax.rem(lax.axis_index('side') + 2, 4)}
    over_x = {'pair': 1 - lax.axis_index('pair')}
    cut = m2_ref.shape[1] // 2

    def plane(k, c):
        mine = (m2_ref, m3_ref)[k]
        if c < 2:
            src, dst = mine, g_ref.at[k, c]
        elif c == 2:
            src, dst = g_ref.at[k, 0, :, pl.ds(0, cut)], g_ref.at[k, 2, :, pl.ds(0, cut)]
        else:
            src, dst = g_ref.at[k, 1, :, pl.ds(cut, cut)], g_ref.at[k, 2, :, pl.ds(cut, cut)]
        return pltpu.make_async_remote_copy(src, dst, gs.at[k, c], gr.at[k, c], device_id=(over_y, over_x, over_x, over_y)[c], device_id_type=mesh_id)

    wcopy(0).start()
    fill = [
        pltpu.make_async_copy(p_ref, a_ref.at[pl.ds(0, 2 * hr)], asem.at[0]),
        pltpu.make_async_copy(q_ref, a_ref.at[pl.ds(2 * hr, q_ref.shape[0])], asem.at[1]),
    ]
    for one in fill:
        one.start()
    line_barrier(zi, zn, (over_y, over_x))

    @pl.when(ends)
    def _():
        for k in range(2):
            for c in range(2):
                plane(k, c).start()

    for one in fill:
        one.wait()

    def take_dn(i):
        @pl.when(zi < zn - 1)
        def _():
            send_dn(i).wait_recv()
            pdn[i] = pdn[i] + rdn[i]

            @pl.when(zi > 0)
            def _():
                send_dn(i).start()

        @pl.when(zi == 0)
        def _():
            cols = pl.ds(pl.multiple_of(i * tn, 128), tn)
            total = pdn[i]
            o_ref[:, cols] = x_ref[:, cols] + total[:hr].astype(jnp.bfloat16)
            ot_ref[:, cols] = (t_ref[:, cols].astype(jnp.bfloat16) + total[hr:].astype(jnp.bfloat16)).astype(jnp.float32)

    def take_up(i):
        @pl.when(zi > 0)
        def _():
            send_up(i).wait_recv()
            pup[i] = pup[i] + rup[i]

            @pl.when(zi < zn - 1)
            def _():
                send_up(i).start()

            cols = pl.ds(pl.multiple_of(i * tn, 128), tn)
            o_ref[:, cols] = x_ref[:, cols] + pup[i].astype(jnp.bfloat16)
            ot_ref[:, cols] = t_ref[:, cols]

    def handle(i):
        def ordered(near, far):
            @pl.when(i < nt)
            def _():
                near(i)

            @pl.when(i > 0)
            def _():
                far(i - 1)

        @pl.when(zi < zn // 2)
        def _():
            ordered(take_up, take_dn)

        @pl.when(zi >= zn // 2)
        def _():
            ordered(take_dn, take_up)

    @pl.loop(0, nt)
    def _(j):
        wcopy(j).wait()

        @pl.when(j + 1 < nt)
        def _():
            wcopy(j + 1).start()

        wt = wbuf[lax.rem(j, 2)]
        part = jnp.dot(a_ref[...], wt, preferred_element_type=jnp.float32)
        pdn[j, :hr] = part[:hr]
        pdn[j, hr:] = part[2 * hr:2 * hr + TOK_PAD]
        pup[j] = part[hr:2 * hr]

        @pl.when(zi == zn - 1)
        def _():
            send_dn(j).start()

        @pl.when(zi == 0)
        def _():
            send_up(j).start()

        @pl.when(j >= lag)
        def _():
            handle(j - lag)

        for k in range(2):
            @pl.when(ends & (j == RELAY_AT[k]))
            def _(k=k):
                plane(k, 0).wait_recv()
                plane(k, 1).wait_recv()
                plane(k, 2).start()
                plane(k, 3).start()

    @pl.loop(nt - lag, nt + 1)
    def _(j):
        handle(j)

    @pl.loop(0, nt)
    def _(j):
        @pl.when(zi > 0)
        def _():
            send_dn(j).wait_send()

        @pl.when(zi < zn - 1)
        def _():
            send_up(j).wait_send()

    @pl.when(ends)
    def _():
        for k in range(2):
            plane(k, 2).wait_recv()
            plane(k, 3).wait_recv()
            for c in range(4):
                plane(k, c).wait_send()


def reduce_call(p_rows, q_rows, x_own, t_own, w_o, m2, m3, zn):
    hr, width = x_own.shape
    depth = p_rows.shape[1]
    total = p_rows.shape[0] + q_rows.shape[0]
    tn = 256
    nt = width // tn
    td = hr + TOK_PAD
    vm = pl.BlockSpec(memory_space=pltpu.VMEM)
    hb = pl.BlockSpec(memory_space=pl.ANY)
    return pl.pallas_call(
        functools.partial(reduce_body, zn, nt, tn, hr),
        out_shape=(
            jax.ShapeDtypeStruct((hr, width), jnp.bfloat16),
            jax.ShapeDtypeStruct((TOK_PAD, width), jnp.float32),
            jax.ShapeDtypeStruct((2, 3) + m2.shape, jnp.bfloat16),
        ),
        in_specs=[hb, hb, vm, vm, hb, hb, hb],
        out_specs=(vm, vm, hb),
        scratch_shapes=[
            pltpu.VMEM((total, depth), jnp.bfloat16),
            dma((2,)),
            dma((2, 4)),
            dma((2, 4)),
            pltpu.VMEM((2, depth, tn), jnp.bfloat16),
            pltpu.VMEM((nt, td, tn), jnp.float32),
            pltpu.VMEM((nt, hr, tn), jnp.float32),
            pltpu.VMEM((nt, td, tn), jnp.float32),
            pltpu.VMEM((nt, hr, tn), jnp.float32),
            dma((2,)),
            dma((nt,)),
            dma((nt,)),
            dma((nt,)),
            dma((nt,)),
        ],
        compiler_params=pltpu.CompilerParams(collective_id=0, has_side_effects=True, vmem_limit_bytes=66_000_000),
        cost_estimate=pl.CostEstimate(flops=2 * total * depth * width, bytes_accessed=depth * width * 2, transcendentals=0),
        name='wo_reduce',
    )(p_rows, q_rows, x_own, t_own, w_o, m2, m3)


def mlp_body(zn, nq, hr, cw, *refs):
    b_ref, h_ref, t_ref, wg_ref, wu_ref, wd_ref = refs[:6]
    half = nq // 2
    n_in = nq + 3
    pieces = refs[6:6 + nq]
    plane_own, spread = refs[6 + nq:8 + nq], refs[8 + nq]
    o_ref, ot_ref, xc_ref, gacc, uacc, m_ref, wbuf, obuf, dbuf, wsem, dsem, xs, xr, sa, ra, sb, rb, st, rt = refs[6 + n_in:]
    zi = lax.axis_index('tp')
    side = lax.axis_index('side')
    qi = lax.axis_index('pair') * (nq // 2) + side
    slots = 4
    steps = slots * nq
    depth = 4

    def flip(e):
        out = 0
        for bit in (1, 2, 4):
            out = out + bit * lax.rem(lax.rem(qi // bit, 2) + lax.rem(e // bit, 2), 2)
        return out

    def cols_at(q):
        return pl.ds(pl.multiple_of(q * cw, 128), cw)

    order = [(s, e) for s in (0, 1) for e in range(nq)]
    order += [(s, e) for par in (0, 1) for s in (2, 3) for e in range(par, nq, 2)]

    def slot_piece(i):
        late = i - 2 * nq
        early = i < 2 * nq
        s = jnp.where(early, i // nq, 2 + lax.rem(late // half, 2))
        e = jnp.where(early, lax.rem(i, nq), 2 * lax.rem(late, half) + late // (2 * half))
        return s, e

    partner = {'side': side + 1 - 2 * lax.rem(side, 2)}

    def at_hand(k, j):
        return plane_own[k] if j == 0 else spread.at[k, j - 1]

    def cross(k, j):
        return pltpu.make_async_remote_copy(at_hand(k, j), xc_ref.at[k, j], xs.at[k, j], xr.at[k, j], device_id=partner, device_id_type=mesh_id)

    def source(s, e):
        if s == 1:
            return pieces[e]
        if e % 2 == 0:
            return at_hand(s - 2, e // 2)
        return xc_ref.at[s - 2, e // 2]

    line_barrier(zi, zn, (partner,))
    ends = (zi == 0) | (zi == zn - 1)

    def start_gu(i):
        buf = lax.rem(i, depth)

        @pl.when(i < nq)
        def _():
            rows = cols_at(flip(i))
            pltpu.make_async_copy(wg_ref.at[rows, :], wbuf.at[buf, 0], wsem.at[buf]).start()
            pltpu.make_async_copy(wu_ref.at[rows, :], wbuf.at[buf, 1], wsem.at[buf]).start()

        for k, (s, e) in enumerate(order):
            if s > 0:
                @pl.when(i == k)
                def _(s=s, e=e):
                    if s > 1 and e % 2:
                        cross(s - 2, e // 2).wait_recv()
                    pltpu.make_async_copy(source(s, e).at[pl.ds(0, 2)], wbuf.at[buf], wsem.at[buf]).start()

    def start_dn(e):
        pltpu.make_async_copy(wd_ref.at[:, cols_at(flip(e))], obuf.at[lax.rem(e, 2)], dsem.at[lax.rem(e, 2), 0]).start()
        for k in range(nq):
            @pl.when(e == k)
            def _(k=k):
                for s in range(1, slots):
                    pltpu.make_async_copy(source(s, k).at[2], dbuf.at[lax.rem(e, 2), s - 1], dsem.at[lax.rem(e, 2), s]).start()

    hh = hr // 2

    def block(h, r, q):
        return o_ref.at[pl.ds(h * hr + r * hh, hh), cols_at(q)]

    def up(q, r):
        return pltpu.make_async_remote_copy(block(0, r, q), block(0, r, q), sa.at[r, q], ra.at[r, q], device_id={'tp': zi + 1}, device_id_type=mesh_id)

    def down(q, r):
        return pltpu.make_async_remote_copy(block(1, r, q), block(1, r, q), sb.at[r, q], rb.at[r, q], device_id={'tp': zi - 1}, device_id_type=mesh_id)

    def tok(q):
        tile = ot_ref.at[:, cols_at(q)]
        return pltpu.make_async_remote_copy(tile, tile, st.at[q], rt.at[q], device_id={'tp': zi + 1}, device_id_type=mesh_id)

    @pl.when(ends)
    def _():
        for k in range(2):
            for j in range(half):
                cross(k, j).start()
        for i in range(depth - 1):
            start_gu(jnp.int32(i))
        gacc[...] = jnp.zeros_like(gacc)
        uacc[...] = jnp.zeros_like(uacc)

        @pl.loop(0, steps)
        def _(i):
            buf = lax.rem(i, depth)
            s, e = slot_piece(i)
            pltpu.make_async_copy(pieces[0].at[pl.ds(0, 2)], wbuf.at[buf], wsem.at[buf]).wait()

            @pl.when(i + depth - 1 < steps)
            def _():
                start_gu(i + depth - 1)

            rows = b_ref[:, cols_at(flip(e))]
            gacc[s] = gacc[s] + jnp.dot(rows, wbuf[buf, 0], preferred_element_type=jnp.float32)
            uacc[s] = uacc[s] + jnp.dot(rows, wbuf[buf, 1], preferred_element_type=jnp.float32)

        start_dn(jnp.int32(0))

        @pl.loop(0, slots)
        def _(s):
            gate = gacc[s]
            m_ref[s] = (gate * jax.nn.sigmoid(gate) * uacc[s]).astype(jnp.bfloat16)

        @pl.loop(0, nq)
        def _(e):
            par = lax.rem(e, 2)
            q = flip(e)
            cols = cols_at(q)

            @pl.when(e + 1 < nq)
            def _():
                start_dn(e + 1)

            acc = None
            for s in range(slots):
                pltpu.make_async_copy(pieces[0].at[2], dbuf.at[par, max(s - 1, 0)], dsem.at[par, s]).wait()
                if s == 0:
                    acc = jnp.dot(m_ref[s], obuf[par], preferred_element_type=jnp.float32)
                else:
                    acc = acc + lax.dot_general(m_ref[s], dbuf[par, s - 1], (((1,), (1,)), ((), ())), preferred_element_type=jnp.float32)
            res = h_ref[:, cols] + acc[:hr].astype(jnp.bfloat16)

            @pl.when(zi == 0)
            def _():
                o_ref[:hr, cols] = res
                ot_ref[:, cols] = (t_ref[:, cols].astype(jnp.bfloat16) + acc[hr:hr + TOK_PAD].astype(jnp.bfloat16)).astype(jnp.float32)
                up(q, 0).start()
                up(q, 1).start()
                tok(q).start()

            @pl.when(zi == zn - 1)
            def _():
                o_ref[hr:, cols] = res
                down(q, 0).start()
                down(q, 1).start()

        for k in range(2):
            for j in range(half):
                cross(k, j).wait_send()

    @pl.when((zi > 0) & (zi < zn - 1))
    def _():
        @pl.loop(0, 2 * nq + 1)
        def _(i):
            def pass_up(n):
                q = flip(n // 2)
                up(q, lax.rem(n, 2)).wait_recv()
                up(q, lax.rem(n, 2)).start()

                @pl.when(lax.rem(n, 2) == 1)
                def _():
                    tok(q).wait_recv()
                    tok(q).start()

            def pass_down(n):
                q = flip(n // 2)
                down(q, lax.rem(n, 2)).wait_recv()
                down(q, lax.rem(n, 2)).start()

            def ordered(near, far):
                @pl.when(i < 2 * nq)
                def _():
                    near(i)

                @pl.when(i > 0)
                def _():
                    far(i - 1)

            @pl.when(zi < zn // 2)
            def _():
                ordered(pass_up, pass_down)

            @pl.when(zi >= zn // 2)
            def _():
                ordered(pass_down, pass_up)

    @pl.loop(0, nq)
    def _(q):
        @pl.when(zi == zn - 1)
        def _():
            up(q, 0).wait_recv()
            up(q, 1).wait_recv()
            tok(q).wait_recv()

        @pl.when(zi == 0)
        def _():
            down(q, 0).wait_recv()
            down(q, 1).wait_recv()

        @pl.when(zi < zn - 1)
        def _():
            up(q, 0).wait_send()
            up(q, 1).wait_send()
            tok(q).wait_send()

        @pl.when(zi > 0)
        def _():
            down(q, 0).wait_send()
            down(q, 1).wait_send()


def mlp_call(b_rows, h_rows, t_rows, w_gate, w_up, w_down, pieces, zn):
    hr, width = h_rows.shape
    br = b_rows.shape[0]
    nq = len(pieces) - 3
    fw = w_gate.shape[1]
    cw = width // nq
    vm = pl.BlockSpec(memory_space=pltpu.VMEM)
    hb = pl.BlockSpec(memory_space=pl.ANY)
    out = pl.pallas_call(
        functools.partial(mlp_body, zn, nq, hr, cw),
        out_shape=(
            jax.ShapeDtypeStruct((2 * hr, width), jnp.bfloat16),
            jax.ShapeDtypeStruct((TOK_PAD, width), jnp.float32),
            jax.ShapeDtypeStruct((2, nq // 2, 3, cw, fw), jnp.bfloat16),
        ),
        in_specs=[vm, vm, vm] + [hb] * (3 + len(pieces)),
        out_specs=(vm, vm, hb),
        scratch_shapes=[
            pltpu.VMEM((4, br, fw), jnp.float32),
            pltpu.VMEM((4, br, fw), jnp.float32),
            pltpu.VMEM((4, br, fw), jnp.bfloat16),
            pltpu.VMEM((4, 2, cw, fw), jnp.bfloat16),
            pltpu.VMEM((2, fw, cw), jnp.bfloat16),
            pltpu.VMEM((2, 3, cw, fw), jnp.bfloat16),
            dma((4,)),
            dma((2, 4)),
            dma((2, nq // 2)),
            dma((2, nq // 2)),
        ] + [dma((2, nq)) for _ in range(4)] + [dma((nq,)) for _ in range(2)],
        compiler_params=pltpu.CompilerParams(collective_id=1, has_side_effects=True, vmem_limit_bytes=60_000_000),
        cost_estimate=pl.CostEstimate(flops=2 * br * 4 * fw * width * 3, bytes_accessed=4 * fw * width * 6, transcendentals=0),
        name='mlp_spread',
    )(b_rows, h_rows, t_rows, w_gate, w_up, w_down, *pieces)
    return out[0], out[1]


def own_piece(w_gate, w_up, w_down, nq):
    qi = lax.axis_index('pair') * (nq // 2) + lax.axis_index('side')
    cw = w_gate.shape[0] // nq
    return jnp.stack([
        lax.dynamic_slice_in_dim(w_gate, qi * cw, cw, 0),
        lax.dynamic_slice_in_dim(w_up, qi * cw, cw, 0),
        lax.dynamic_slice_in_dim(w_down, qi * cw, cw, 1).T,
    ])


def to_ends(piece, step, zn):
    return lax.ppermute(piece, 'tp', [(step, 0), (zn - 1 - step, zn - 1)])


def plane_step(mine):
    over_y = lax.ppermute(mine, 'side', [(0, 2), (2, 0), (1, 3), (3, 1)])
    over_x = lax.ppermute(mine, 'pair', [(0, 1), (1, 0)])
    over_d = lax.ppermute(mine, ('pair', 'side'), [(p * 4 + s, (1 - p) * 4 + (s + 2) % 4) for p in range(2) for s in range(4)])
    return [mine, over_y, over_x, over_d]


def core_step(parts):
    out = []
    for part in parts:
        out += [part, lax.ppermute(part, 'side', [(0, 1), (1, 0), (2, 3), (3, 2)])]
    return out


def tie(*values):
    return lax.optimization_barrier(values)


def solution(mesh):
    groups = mesh.shape['side']
    zn = mesh.shape['tp']
    nq = mesh.shape['pair'] * groups
    shift_pairs = [(source_idx, (source_idx + 1) % groups) for source_idx in range(groups)]
    group_axes = ('pair', 'side')
    head_spec = P(none, none, 'tp', none)
    cache_spec = P(group_axes, none, none, none, 'tp', none)
    prompt_spec = P(group_axes, none, none, 'tp', none)
    row_spec = P(group_axes, none, none)
    spec_in = (row_spec, P(group_axes), row_spec, cache_spec, cache_spec, P(group_axes, none), P(), head_spec, P(), head_spec, head_spec, P(none, 'tp', none, none), P(), P(none, none, 'tp'), P(none, none, 'tp'), P(none, 'tp', none))
    spec_out = (row_spec, row_spec, prompt_spec, prompt_spec, cache_spec, cache_spec)

    def device_step(x_prompt, s_len, y_tok, k_cache, v_cache, c_len, attn_gain, w_q, w_dkv, w_uk, w_uv, w_o, mlp_gain, w_gate, w_up, w_down):
        layer = (attn_gain, w_q, w_dkv, w_uk, w_uv, w_o, mlp_gain, w_gate, w_up, w_down)
        attn_gain, w_q, w_dkv, w_uk, w_uv, w_o, mlp_gain, w_gate, w_up, w_down = (v[0] for v in layer)
        zi = lax.axis_index('tp')
        hidden, toks = x_prompt[0], y_tok[0]
        rows, width = hidden.shape
        nb = toks.shape[0]
        hr = rows // 2
        cur_len = c_len[0]
        own = own_piece(w_gate, w_up, w_down, nq)
        near = to_ends(own, 1, zn)

        every = jnp.concatenate([hidden, toks, jnp.zeros((16 - nb, width), hidden.dtype)], axis=0)
        positions = jnp.concatenate([jnp.arange(rows, dtype=jnp.int32), cur_len, jnp.zeros((16 - nb,), jnp.int32)])
        normed = rms_scaled(every, attn_gain)
        latent_pack = make_latent(normed, w_dkv, positions, w_uk.shape[0])
        received = lax.ppermute(latent_pack[:rows], 'side', shift_pairs)
        nope, rank = w_uk.shape[-1], w_uk.shape[0]
        heads, rope = w_q.shape[1], w_q.shape[2] - nope
        latent, rope_key = latent_pack[:, :rank], latent_pack[:, rank:]
        key_t = jnp.einsum('sr,rhn->hns', latent, w_uk, preferred_element_type=jnp.float32).astype(jnp.bfloat16)
        value = jnp.einsum('sr,rhv->hsv', latent, w_uv, preferred_element_type=jnp.float32).astype(jnp.bfloat16)
        cos, sin = rope_tables(positions, rope)
        rope_t = jnp.concatenate([rope_key[:rows].T] * 2, axis=0)
        normed, own, near = tie(normed, own, near)
        first = plane_step(near)
        middle = to_ends(own, 2, zn)
        far = to_ends(own, 3, zn)
        p_rows, q_tok = attend_call(normed, w_q.transpose(1, 2, 0), key_t, rope_t, value, cos, sin, s_len, rows, w_q.shape[2] ** -0.5)

        q_rope = q_tok[:, :nb, nope:nope + rope] + q_tok[:, :nb, nope + rope:]
        query_tok = jnp.concatenate([q_tok[:, :nb, :nope], q_rope], axis=-1).transpose(1, 0, 2)
        rope_new = jnp.broadcast_to(rope_key[rows:rows + nb, None, :], (nb, heads, rope))
        key_new = jnp.concatenate([key_t[:, :, rows:rows + nb].transpose(2, 0, 1), rope_new], axis=-1)
        value_new = value[:, rows:rows + nb].transpose(1, 0, 2)
        key_old, value_old = k_cache[0, 0], v_cache[0, 0]
        slot_hit = (jnp.arange(key_old.shape[1])[None, :] == cur_len[:, None])[:, :, None, None]
        key_layer = jnp.where(slot_hit, key_new[:, None], key_old)
        value_layer = jnp.where(slot_hit, value_new[:, None], value_old)
        tok_val = cache_attention(query_tok, key_layer, value_layer, cur_len).reshape(nb, -1)
        q_rows = jnp.concatenate([tok_val, jnp.zeros((16 - nb, tok_val.shape[1]), tok_val.dtype)], axis=0)

        p_rows, received = tie(p_rows, received)
        x_own = lax.dynamic_slice_in_dim(hidden, jnp.where(zi < zn // 2, 0, hr), hr, 0)
        t_own = jnp.concatenate([toks, jnp.zeros((TOK_PAD - nb, width), toks.dtype)], axis=0).astype(jnp.float32)
        h_mid, t_mid, spread = reduce_call(p_rows, q_rows, x_own, t_own, w_o.reshape(-1, width), middle, far, zn)
        h_mid, first = tie(h_mid, first)
        pieces = core_step(first) + [middle, far, spread]

        key_in, value_in = expand_latent(received, w_uk, w_uv)

        b_rows = jnp.concatenate([
            rms_scaled(h_mid, mlp_gain),
            rms_scaled(t_mid.astype(jnp.bfloat16), mlp_gain),
            jnp.zeros((TOK_PAD, width), jnp.bfloat16),
        ], axis=0)
        h_out, t_out = mlp_call(b_rows, h_mid, t_mid, w_gate, w_up, w_down, pieces, zn)
        y_out = t_out[:nb].astype(jnp.bfloat16)
        return (h_out[None], y_out[None], key_in[None, None], value_in[None, None], key_layer[None, None], value_layer[None, None])

    return jax.shard_map(device_step, mesh=mesh, in_specs=spec_in, out_specs=spec_out, check_vma=False)
```

```python
import functools
import jax
import jax.numpy as jnp
from jax import lax
from jax.experimental import pallas as pl
from jax.experimental.pallas import tpu as pltpu
from jax.sharding import PartitionSpec as P

EPSILON = 1e-6
THETA = 10000.0
TOK_PAD = 8
BITS = (1, 2, 4)
dma = pltpu.SemaphoreType.DMA
mesh_id = pl.DeviceIdType.MESH
none = None
END_LAG = 6
RELAY_AT = (12, 21)
MID_LAG = 2


def odd(value):
    return lax.rem(value, 2)


def rms_plain(values):
    hidden = values.astype(jnp.float32)
    inv_rms = lax.rsqrt(jnp.mean(hidden * hidden, axis=-1, keepdims=True) + EPSILON)
    return (hidden * inv_rms).astype(jnp.bfloat16)


def apply_rope(values, positions):
    half_dim = values.shape[-1] // 2
    inv_freq = THETA ** (-jnp.arange(half_dim, dtype=jnp.float32) * 2.0 / values.shape[-1])
    angles = positions.astype(jnp.float32)[..., None] * inv_freq
    cos_part = jnp.cos(angles)
    sin_part = jnp.sin(angles)
    first_half = values[..., :half_dim].astype(jnp.float32)
    second_half = values[..., half_dim:].astype(jnp.float32)
    return jnp.concatenate([first_half * cos_part - second_half * sin_part, second_half * cos_part + first_half * sin_part], axis=-1).astype(jnp.bfloat16)


def rope_tables(positions, rope_dim):
    half_dim = rope_dim // 2
    inv_freq = THETA ** (-jnp.arange(half_dim, dtype=jnp.float32) * 2.0 / rope_dim)
    angles = positions.astype(jnp.float32)[..., None] * inv_freq
    return jnp.tile(jnp.cos(angles), (1, 4)), jnp.tile(jnp.sin(angles), (1, 4))


def finish_latent(latent_raw, positions, rank_dim):
    return jnp.concatenate([rms_plain(latent_raw[:, :rank_dim]), apply_rope(latent_raw[:, rank_dim:], positions)], axis=-1)


def expand_keys(latent_pack, w_uk_layer):
    rank_dim = w_uk_layer.shape[0]
    rope_key = latent_pack[:, rank_dim:]
    key_nope = jnp.einsum('sr,rhn->shn', latent_pack[:, :rank_dim], w_uk_layer, preferred_element_type=jnp.float32).astype(jnp.bfloat16)
    rope_heads = jnp.broadcast_to(rope_key[:, None, :], (key_nope.shape[0], key_nope.shape[1], rope_key.shape[1]))
    return jnp.concatenate([key_nope, rope_heads], axis=-1)


def expand_values(latent_pack, w_uv_layer):
    return jnp.einsum('sr,rhv->shv', latent_pack[:, :w_uv_layer.shape[0]], w_uv_layer, preferred_element_type=jnp.float32).astype(jnp.bfloat16)


def masked_softmax(scores, allowed):
    return jax.nn.softmax(jnp.where(allowed, scores, -1e30), axis=-1).astype(jnp.bfloat16)


def cache_attention(query_all, key_layer, value_layer, cur_len):
    scores = jnp.einsum('bhe,bthe->bht', query_all, key_layer, preferred_element_type=jnp.float32) * query_all.shape[-1] ** -0.5
    allowed = jnp.arange(key_layer.shape[1])[None, None, :] <= cur_len[:, None, None]
    probs_bf = masked_softmax(scores, allowed)
    return jnp.einsum('bht,bthv->bhv', probs_bf, value_layer, preferred_element_type=jnp.float32).astype(jnp.bfloat16)


def line_barrier(zi, zn, also):
    sem = pltpu.get_barrier_semaphore()

    for one in also:
        pl.semaphore_signal(sem, inc=1, device_id=one, device_id_type=mesh_id)

    @pl.when(zi > 0)
    def _():
        pl.semaphore_signal(sem, inc=1, device_id={'tp': zi - 1}, device_id_type=mesh_id)

    @pl.when(zi < zn - 1)
    def _():
        pl.semaphore_signal(sem, inc=1, device_id={'tp': zi + 1}, device_id_type=mesh_id)

    @pl.when((zi == 0) | (zi == zn - 1))
    def _():
        pl.semaphore_wait(sem, 1 + len(also))

    @pl.when((zi > 0) & (zi < zn - 1))
    def _():
        pl.semaphore_wait(sem, 2 + len(also))


def latent_body(x_ref, t_ref, gain_ref, w_ref, n_ref, raw_ref, acc):
    rows, depth = x_ref.shape
    step = t_ref.shape[0]
    chunk = depth // 4

    def norm(x):
        x = x.astype(jnp.float32)
        inv = lax.rsqrt(jnp.mean(x * x, axis=-1, keepdims=True) + EPSILON)
        return (x * inv * gain_ref[...]).astype(jnp.bfloat16)

    @pl.loop(0, rows // step)
    def _(r):
        span = pl.ds(pl.multiple_of(r * step, step), step)
        n_ref[span] = norm(x_ref[span])

    n_ref[rows:] = norm(t_ref[...])
    acc[...] = jnp.zeros_like(acc)

    @pl.loop(0, 4)
    def _(c):
        span = pl.ds(pl.multiple_of(c * chunk, chunk), chunk)
        acc[...] = acc[...] + lax.dot_general(n_ref[:, span], w_ref[:, span], (((1,), (1,)), ((), ())), preferred_element_type=jnp.float32)

    raw_ref[...] = acc[...].astype(jnp.bfloat16)


def latent_call(x_rows, t_rows, gain, w_dkv):
    total = x_rows.shape[0] + t_rows.shape[0]
    feat, depth = w_dkv.shape
    vm = pl.BlockSpec(memory_space=pltpu.VMEM)
    return pl.pallas_call(
        latent_body,
        out_shape=(jax.ShapeDtypeStruct((total, depth), jnp.bfloat16), jax.ShapeDtypeStruct((total, feat), jnp.bfloat16)),
        in_specs=[vm] * 4,
        out_specs=(vm, vm),
        scratch_shapes=[pltpu.VMEM((total, feat), jnp.float32)],
        compiler_params=pltpu.CompilerParams(vmem_limit_bytes=40_000_000),
        cost_estimate=pl.CostEstimate(flops=2 * total * depth * feat, bytes_accessed=depth * (feat + 2 * total) * 2, transcendentals=0),
        name='latent',
    )(x_rows, t_rows, gain, w_dkv)


def attend_body(rows, nope, rope, scale, n_ref, w_ref, k_ref, r_ref, v_ref, cos_ref, sin_ref, len_ref, o_ref, qt_ref, acc):
    heads = w_ref.shape[0]
    depth = n_ref.shape[1]
    chunk = depth // 4
    lane = lax.broadcasted_iota(jnp.int32, (1, 2 * rope), 1)
    low = lane < rope
    first = lax.rem(lane, rope) < rope // 2
    wide = heads * (nope + rope)

    def part(c):
        span = pl.ds(pl.multiple_of(c * chunk, 128), chunk)
        return lax.dot_general(n_ref[:, span], w_ref[:, :, span].reshape(wide, chunk), (((1,), (1,)), ((), ())), preferred_element_type=jnp.float32)

    acc[...] = part(0)

    @pl.loop(1, 4)
    def _(c):
        acc[...] = acc[...] + part(c)

    cos, sin = cos_ref[...], sin_ref[...]
    valid = len_ref[0]
    kr = r_ref[...]
    half_rows = rows // 2

    @pl.loop(0, heads // 2)
    def _(pair):
        t0, t1, t2 = (acc[:, pl.ds(pl.multiple_of((pair * 3 + i) * nope, nope), nope)].astype(jnp.bfloat16).astype(jnp.float32) for i in range(3))
        n1 = jnp.where(low, pltpu.roll(t1, rope, 1), pltpu.roll(t2, rope, 1))
        both = jnp.where(low, t1, t2)
        turned = jnp.where(first, -pltpu.roll(both, 2 * rope - rope // 2, 1), pltpu.roll(both, rope // 2, 1))
        both = both * cos + turned * sin
        for sub, nq in ((0, t0), (1, n1)):
            h = pair * 2 + sub
            keep = low if sub == 0 else jnp.logical_not(low)
            query = jnp.concatenate([nq.astype(jnp.bfloat16), jnp.where(keep, both, 0.0).astype(jnp.bfloat16)], axis=1)
            qt_ref[h] = query[rows:]
            for blk in range(2):
                span = (blk + 1) * half_rows
                key = jnp.concatenate([k_ref[h, :span], kr[:span]], axis=1)
                s = lax.dot_general(query[blk * half_rows:(blk + 1) * half_rows], key, (((1,), (1,)), ((), ())), preferred_element_type=jnp.float32) * scale
                row = lax.broadcasted_iota(jnp.int32, s.shape, 0) + blk * half_rows
                col = lax.broadcasted_iota(jnp.int32, s.shape, 1)
                s = jnp.where((col <= row) & (col < valid), s, -1e30)
                p = jnp.exp(s - jnp.max(s, axis=1, keepdims=True))
                p = (p * (1.0 / jnp.sum(p, axis=1, keepdims=True))).astype(jnp.bfloat16)
                out = jnp.dot(p, v_ref[h, :span, :], preferred_element_type=jnp.float32)
                o_ref[blk * half_rows:(blk + 1) * half_rows, pl.ds(pl.multiple_of(h * nope, nope), nope)] = out.astype(jnp.bfloat16)


def attend_call(normed, w_q, key_all, rope_two, value, cos, sin, valid_len, rows, scale):
    total, depth = normed.shape
    heads, feat, _ = w_q.shape
    nope = key_all.shape[2]
    rope = feat - nope
    vdim = value.shape[2]
    grp = 4
    vm = pl.BlockSpec(memory_space=pltpu.VMEM)
    return pl.pallas_call(
        functools.partial(attend_body, rows, nope, rope, scale),
        grid=(heads // grp,),
        out_shape=(jax.ShapeDtypeStruct((rows, heads * vdim), jnp.bfloat16), jax.ShapeDtypeStruct((heads, total - rows, 2 * nope), jnp.bfloat16)),
        in_specs=[
            vm,
            pl.BlockSpec((grp, feat, depth), lambda g: (g, 0, 0)),
            pl.BlockSpec((grp, key_all.shape[1], nope), lambda g: (g, 0, 0)),
            vm,
            pl.BlockSpec((grp, value.shape[1], vdim), lambda g: (g, 0, 0)),
            vm, vm,
            pl.BlockSpec(memory_space=pltpu.SMEM),
        ],
        out_specs=(pl.BlockSpec((rows, grp * vdim), lambda g: (0, g)), pl.BlockSpec((grp, total - rows, 2 * nope), lambda g: (g, 0, 0))),
        scratch_shapes=[pltpu.VMEM((total, grp * feat), jnp.float32)],
        compiler_params=pltpu.CompilerParams(vmem_limit_bytes=60_000_000),
        cost_estimate=pl.CostEstimate(flops=2 * total * depth * heads * feat + 3 * rows * rows * heads * feat, bytes_accessed=heads * feat * depth * 2, transcendentals=rows * rows * heads),
        name='attend',
    )(normed, w_q, key_all, rope_two, value, cos, sin, valid_len)


def reduce_body(zn, nt, tn, hr, p_ref, q_ref, x_ref, t_ref, w_ref, f0_ref, f1_ref, f2_ref, f3_ref, m2_ref, m3_ref, o_ref, ot_ref, g_ref, xc_ref, a_ref, asem, gs, gr, xs, xr, wbuf, pdn, pup, rdn, rup, wsem, sdn, sup, vdn, vup):
    zi = lax.axis_index('tp')

    def wcopy(j):
        return pltpu.make_async_copy(w_ref.at[:, pl.ds(pl.multiple_of(j * tn, 128), tn)], wbuf.at[odd(j)], wsem.at[odd(j)])

    def send_dn(i):
        return pltpu.make_async_remote_copy(pdn.at[i], rdn.at[i], sdn.at[i], vdn.at[i], device_id={'tp': zi - 1}, device_id_type=mesh_id)

    def send_up(i):
        return pltpu.make_async_remote_copy(pup.at[i], rup.at[i], sup.at[i], vup.at[i], device_id={'tp': zi + 1}, device_id_type=mesh_id)

    ends = (zi == 0) | (zi == zn - 1)
    lag = jnp.where(ends, END_LAG, MID_LAG)
    over_y = {'side': lax.rem(lax.axis_index('side') + 2, 4)}
    over_x = {'pair': 1 - lax.axis_index('pair')}
    cut = m2_ref.shape[1] // 2

    def plane(k, c):
        mine = (m2_ref, m3_ref)[k]
        if c < 2:
            src, dst = mine, g_ref.at[k, c]
        elif c == 2:
            src, dst = g_ref.at[k, 0, :, pl.ds(0, cut)], g_ref.at[k, 2, :, pl.ds(0, cut)]
        else:
            src, dst = g_ref.at[k, 1, :, pl.ds(cut, cut)], g_ref.at[k, 2, :, pl.ds(cut, cut)]
        return pltpu.make_async_remote_copy(src, dst, gs.at[k, c], gr.at[k, c], device_id=(over_y, over_x, over_x, over_y)[c], device_id_type=mesh_id)

    side = lax.axis_index('side')
    partner = {'side': side + 1 - 2 * odd(side)}

    def cross(k, c):
        if k == 0:
            src = (f0_ref, f1_ref, f2_ref, f3_ref)[c]
        elif c == 0:
            src = (m2_ref, m3_ref)[k - 1]
        else:
            src = g_ref.at[k - 1, c - 1]
        return pltpu.make_async_remote_copy(src, xc_ref.at[k, c], xs.at[k, c], xr.at[k, c], device_id=partner, device_id_type=mesh_id)

    crossed = [(k, c) for k in range(3) for c in range(4) if k + c < 5]

    wcopy(0).start()
    fill = [
        pltpu.make_async_copy(p_ref, a_ref.at[pl.ds(0, 2 * hr)], asem.at[0]),
        pltpu.make_async_copy(q_ref, a_ref.at[pl.ds(2 * hr, q_ref.shape[0])], asem.at[1]),
    ]
    for one in fill:
        one.start()
    line_barrier(zi, zn, (over_y, over_x, partner))

    @pl.when(ends)
    def _():
        for k in range(2):
            for c in range(2):
                plane(k, c).start()
        for k, c in crossed:
            if k * c == 0:
                cross(k, c).start()

    for one in fill:
        one.wait()

    def take_dn(i):
        @pl.when(zi < zn - 1)
        def _():
            send_dn(i).wait_recv()
            pdn[i] = pdn[i] + rdn[i]

            @pl.when(zi > 0)
            def _():
                send_dn(i).start()

        @pl.when(zi == 0)
        def _():
            cols = pl.ds(pl.multiple_of(i * tn, 128), tn)
            total = pdn[i]
            o_ref[:, cols] = x_ref[:, cols] + total[:hr].astype(jnp.bfloat16)
            ot_ref[:, cols] = (t_ref[:, cols].astype(jnp.bfloat16) + total[hr:].astype(jnp.bfloat16)).astype(jnp.float32)

    def take_up(i):
        @pl.when(zi > 0)
        def _():
            send_up(i).wait_recv()
            pup[i] = pup[i] + rup[i]

            @pl.when(zi < zn - 1)
            def _():
                send_up(i).start()

            cols = pl.ds(pl.multiple_of(i * tn, 128), tn)
            o_ref[:, cols] = x_ref[:, cols] + pup[i].astype(jnp.bfloat16)
            ot_ref[:, cols] = t_ref[:, cols]

    def handle(i):
        def ordered(near, far):
            @pl.when(i < nt)
            def _():
                near(i)

            @pl.when(i > 0)
            def _():
                far(i - 1)

        @pl.when(zi < zn // 2)
        def _():
            ordered(take_up, take_dn)

        @pl.when(zi >= zn // 2)
        def _():
            ordered(take_dn, take_up)

    @pl.loop(0, nt)
    def _(j):
        wcopy(j).wait()

        @pl.when(j + 1 < nt)
        def _():
            wcopy(j + 1).start()

        wt = wbuf[odd(j)]
        part = jnp.dot(a_ref[...], wt, preferred_element_type=jnp.float32)
        pdn[j, :hr] = part[:hr]
        pdn[j, hr:] = part[2 * hr:2 * hr + TOK_PAD]
        pup[j] = part[hr:2 * hr]

        @pl.when(zi == zn - 1)
        def _():
            send_dn(j).start()

        @pl.when(zi == 0)
        def _():
            send_up(j).start()

        @pl.when(j >= lag)
        def _():
            handle(j - lag)

        for k in range(2):
            @pl.when(ends & (j == RELAY_AT[k]))
            def _(k=k):
                plane(k, 0).wait_recv()
                plane(k, 1).wait_recv()
                plane(k, 2).start()
                plane(k, 3).start()
                cross(k + 1, 1).start()
                cross(k + 1, 2).start()

    @pl.loop(nt - lag, nt + 1)
    def _(j):
        handle(j)

    @pl.loop(0, nt)
    def _(j):
        @pl.when(zi > 0)
        def _():
            send_dn(j).wait_send()

        @pl.when(zi < zn - 1)
        def _():
            send_up(j).wait_send()

    @pl.when(ends)
    def _():
        for k in range(2):
            plane(k, 2).wait_recv()
            plane(k, 3).wait_recv()
            if k == 0:
                cross(1, 3).start()
            for c in range(4):
                plane(k, c).wait_send()
        for k, c in crossed:
            cross(k, c).wait()


def reduce_call(p_rows, q_rows, x_own, t_own, w_o, first, m2, m3, zn):
    hr, width = x_own.shape
    depth = p_rows.shape[1]
    total = p_rows.shape[0] + q_rows.shape[0]
    tn = 256
    nt = width // tn
    td = hr + TOK_PAD
    vm = pl.BlockSpec(memory_space=pltpu.VMEM)
    hb = pl.BlockSpec(memory_space=pl.ANY)
    return pl.pallas_call(
        functools.partial(reduce_body, zn, nt, tn, hr),
        out_shape=(
            jax.ShapeDtypeStruct((hr, width), jnp.bfloat16),
            jax.ShapeDtypeStruct((TOK_PAD, width), jnp.float32),
            jax.ShapeDtypeStruct((2, 3) + m2.shape, jnp.bfloat16),
            jax.ShapeDtypeStruct((3, 4) + m2.shape, jnp.bfloat16),
        ),
        in_specs=[hb, hb, vm, vm] + [hb] * 7,
        out_specs=(vm, vm, hb, hb),
        scratch_shapes=[
            pltpu.VMEM((total, depth), jnp.bfloat16),
            dma((2,)),
            *[dma((n, 4)) for n in (2, 2, 3, 3)],
            pltpu.VMEM((2, depth, tn), jnp.bfloat16),
            pltpu.VMEM((nt, td, tn), jnp.float32),
            pltpu.VMEM((nt, hr, tn), jnp.float32),
            pltpu.VMEM((nt, td, tn), jnp.float32),
            pltpu.VMEM((nt, hr, tn), jnp.float32),
            dma((2,)),
            dma((nt,)),
            dma((nt,)),
            dma((nt,)),
            dma((nt,)),
        ],
        compiler_params=pltpu.CompilerParams(collective_id=0, has_side_effects=True, vmem_limit_bytes=66_000_000),
        cost_estimate=pl.CostEstimate(flops=2 * total * depth * width, bytes_accessed=depth * width * 2, transcendentals=0),
        name='wo_reduce',
    )(p_rows, q_rows, x_own, t_own, w_o, *first, m2, m3)


def mlp_body(zn, nq, hr, cw, *refs):
    h_ref, t_ref, gain_ref, wg_ref, wu_ref, wd_ref = refs[:6]
    half = nq // 2
    n_in = half + 4
    first = refs[6:6 + half]
    plane_own = refs[6 + half:8 + half]
    spread, crossed = refs[8 + half:6 + n_in]
    o_ref, ot_ref, xl_ref, b_ref, gacc, uacc, m_ref, wbuf, obuf, dbuf, wsem, dsem, xs, xr, sa, ra, sb, rb, st, rt = refs[6 + n_in:]
    zi = lax.axis_index('tp')
    side = lax.axis_index('side')
    qi = lax.axis_index('pair') * (nq // 2) + side
    slots = 4
    depth = wbuf.shape[0]

    def flip(e):
        out = 0
        for bit in BITS:
            out = out + bit * odd(lax.rem(qi // bit, 2) + lax.rem(e // bit, 2))
        return out

    def cols_at(q):
        return pl.ds(pl.multiple_of(q * cw, 128), cw)

    two = range(2)
    order = [(s, e, e + 1) for s in two for e in range(0, nq, 2)]
    order += [(s + 2, e, e + 2) for par in two for s in two for e in range(par, nq, 4)]
    steps = len(order)

    def slot_pieces(i):
        late = i - nq
        early = i < nq
        s = jnp.where(early, i // half, 2 + odd(late // 2))
        ea = jnp.where(early, 2 * lax.rem(i, half), 4 * odd(late) + late // half)
        return s, ea, ea + jnp.where(early, 1, 2)

    partner = {'side': side + 1 - 2 * odd(side)}

    def at_hand(k, j):
        return plane_own[k] if j == 0 else spread.at[k, j - 1]

    last = pltpu.make_async_remote_copy(at_hand(1, half - 1), xl_ref, xs, xr, device_id=partner, device_id_type=mesh_id)

    def source(s, e):
        if e % 2:
            return xl_ref if (s, e) == (slots - 1, nq - 1) else crossed.at[s - 1, e // 2]
        return first[e // 2] if s == 1 else at_hand(s - 2, e // 2)

    line_barrier(zi, zn, (partner,))
    ends = (zi == 0) | (zi == zn - 1)

    def start_gu(i):
        buf = lax.rem(i, depth)

        @pl.when(i < half)
        def _():
            for h in two:
                rows = cols_at(flip(2 * i + h))
                pltpu.make_async_copy(wg_ref.at[rows, :], wbuf.at[buf, 0, pl.ds(h * cw, cw)], wsem.at[buf]).start()
                pltpu.make_async_copy(wu_ref.at[rows, :], wbuf.at[buf, 1, pl.ds(h * cw, cw)], wsem.at[buf]).start()

        for k, (s, *es) in enumerate(order):
            if s > 0:
                @pl.when(i == k)
                def _(s=s, es=es):
                    for h, e in enumerate(es):
                        if (s, e) == (slots - 1, nq - 1):
                            last.wait_recv()
                        pltpu.make_async_copy(source(s, e).at[pl.ds(0, 2)], wbuf.at[buf, :, pl.ds(h * cw, cw)], wsem.at[buf]).start()

    def start_dn(e):
        pltpu.make_async_copy(wd_ref.at[:, cols_at(flip(e))], obuf.at[odd(e)], dsem.at[odd(e), 0]).start()
        for k in range(nq):
            @pl.when(e == k)
            def _(k=k):
                for s in range(1, slots):
                    pltpu.make_async_copy(source(s, k).at[2], dbuf.at[odd(e), s - 1], dsem.at[odd(e), s]).start()

    hh = hr // 2

    def block(h, r, q):
        return o_ref.at[pl.ds(h * hr + r * hh, hh), cols_at(q)]

    def up(q, r):
        return pltpu.make_async_remote_copy(block(0, r, q), block(0, r, q), sa.at[r, q], ra.at[r, q], device_id={'tp': zi + 1}, device_id_type=mesh_id)

    def down(q, r):
        return pltpu.make_async_remote_copy(block(1, r, q), block(1, r, q), sb.at[r, q], rb.at[r, q], device_id={'tp': zi - 1}, device_id_type=mesh_id)

    def tok(q):
        tile = ot_ref.at[:, cols_at(q)]
        return pltpu.make_async_remote_copy(tile, tile, st.at[q], rt.at[q], device_id={'tp': zi + 1}, device_id_type=mesh_id)

    @pl.when(ends)
    def _():
        last.start()
        for i in range(depth - 1):
            start_gu(jnp.int32(i))

        def norm(x):
            inv = lax.rsqrt(jnp.mean(x * x, axis=-1, keepdims=True) + EPSILON)
            return (x * inv * gain_ref[...]).astype(jnp.bfloat16)

        @pl.loop(0, hr // 16)
        def _(r):
            span = pl.ds(pl.multiple_of(r * 16, 16), 16)
            b_ref[span] = norm(h_ref[span].astype(jnp.float32))

        b_ref[hr:] = norm(jnp.concatenate([t_ref[...]] * 2, axis=0))
        gacc[...] = jnp.zeros_like(gacc)
        uacc[...] = jnp.zeros_like(uacc)

        @pl.loop(0, steps)
        def _(i):
            buf = lax.rem(i, depth)
            s, ea, eb = slot_pieces(i)
            pltpu.make_async_copy(wbuf.at[buf], wbuf.at[buf], wsem.at[buf]).wait()

            @pl.when(i + depth - 1 < steps)
            def _():
                start_gu(i + depth - 1)

            rows = jnp.concatenate([b_ref[:, cols_at(flip(ea))], b_ref[:, cols_at(flip(eb))]], axis=1)
            gacc[s] = gacc[s] + jnp.dot(rows, wbuf[buf, 0], preferred_element_type=jnp.float32)
            uacc[s] = uacc[s] + jnp.dot(rows, wbuf[buf, 1], preferred_element_type=jnp.float32)

        start_dn(jnp.int32(0))

        @pl.loop(0, slots)
        def _(s):
            gate = gacc[s]
            m_ref[s] = (gate * jax.nn.sigmoid(gate) * uacc[s]).astype(jnp.bfloat16)

        @pl.loop(0, nq)
        def _(e):
            par = odd(e)
            q = flip(e)
            cols = cols_at(q)

            @pl.when(e + 1 < nq)
            def _():
                start_dn(e + 1)

            acc = None
            for s in range(slots):
                pltpu.make_async_copy(first[0].at[2], dbuf.at[par, max(s - 1, 0)], dsem.at[par, s]).wait()
                if s == 0:
                    acc = jnp.dot(m_ref[s], obuf[par], preferred_element_type=jnp.float32)
                else:
                    acc = acc + lax.dot_general(m_ref[s], dbuf[par, s - 1], (((1,), (1,)), ((), ())), preferred_element_type=jnp.float32)
            res = h_ref[:, cols] + acc[:hr].astype(jnp.bfloat16)

            @pl.when(zi == 0)
            def _():
                o_ref[:hr, cols] = res
                ot_ref[:, cols] = (t_ref[:, cols].astype(jnp.bfloat16) + acc[hr:hr + TOK_PAD].astype(jnp.bfloat16)).astype(jnp.float32)
                for r in two:
                    up(q, r).start()
                tok(q).start()

            @pl.when(zi == zn - 1)
            def _():
                o_ref[hr:, cols] = res
                for r in two:
                    down(q, r).start()

        last.wait_send()

    @pl.when((zi > 0) & (zi < zn - 1))
    def _():
        @pl.loop(0, 2 * nq + 1)
        def _(i):
            def pass_up(n):
                q = flip(n // 2)
                up(q, odd(n)).wait_recv()
                up(q, odd(n)).start()

                @pl.when(odd(n) == 1)
                def _():
                    tok(q).wait_recv()
                    tok(q).start()

            def pass_down(n):
                q = flip(n // 2)
                down(q, odd(n)).wait_recv()
                down(q, odd(n)).start()

            def ordered(near, far):
                @pl.when(i < 2 * nq)
                def _():
                    near(i)

                @pl.when(i > 0)
                def _():
                    far(i - 1)

            @pl.when(zi < zn // 2)
            def _():
                ordered(pass_up, pass_down)

            @pl.when(zi >= zn // 2)
            def _():
                ordered(pass_down, pass_up)

    @pl.loop(0, nq)
    def _(q):
        @pl.when(zi == zn - 1)
        def _():
            for r in two:
                up(q, r).wait_recv()
            tok(q).wait_recv()

        @pl.when(zi == 0)
        def _():
            for r in two:
                down(q, r).wait_recv()

        @pl.when(zi < zn - 1)
        def _():
            for r in two:
                up(q, r).wait_send()
            tok(q).wait_send()

        @pl.when(zi > 0)
        def _():
            for r in two:
                down(q, r).wait_send()


def mlp_call(h_rows, t_rows, gain, w_gate, w_up, w_down, pieces, zn):
    hr, width = h_rows.shape
    br = hr + 2 * TOK_PAD
    nq = 2 * (len(pieces) - 4)
    fw = w_gate.shape[1]
    cw = width // nq
    vm = pl.BlockSpec(memory_space=pltpu.VMEM)
    hb = pl.BlockSpec(memory_space=pl.ANY)
    out = pl.pallas_call(
        functools.partial(mlp_body, zn, nq, hr, cw),
        out_shape=(
            jax.ShapeDtypeStruct((2 * hr, width), jnp.bfloat16),
            jax.ShapeDtypeStruct((TOK_PAD, width), jnp.float32),
            jax.ShapeDtypeStruct((3, cw, fw), jnp.bfloat16),
        ),
        in_specs=[vm, vm, vm] + [hb] * (3 + len(pieces)),
        out_specs=(vm, vm, hb),
        scratch_shapes=[
            pltpu.VMEM((br, width), jnp.bfloat16),
            pltpu.VMEM((4, br, fw), jnp.float32),
            pltpu.VMEM((4, br, fw), jnp.float32),
            pltpu.VMEM((4, br, fw), jnp.bfloat16),
            pltpu.VMEM((3, 2, 2 * cw, fw), jnp.bfloat16),
            pltpu.VMEM((2, fw, cw), jnp.bfloat16),
            pltpu.VMEM((2, 3, cw, fw), jnp.bfloat16),
            dma((3,)),
            dma((2, 4)),
            dma,
            dma,
        ] + [dma((2, nq)) for _ in range(4)] + [dma((nq,)) for _ in range(2)],
        compiler_params=pltpu.CompilerParams(collective_id=1, has_side_effects=True, vmem_limit_bytes=60_000_000),
        cost_estimate=pl.CostEstimate(flops=2 * br * 4 * fw * width * 3, bytes_accessed=4 * fw * width * 6, transcendentals=0),
        name='mlp_spread',
    )(h_rows, t_rows, gain, w_gate, w_up, w_down, *pieces)
    return out[0], out[1]


def own_piece(w_gate, w_up, w_down, nq):
    qi = lax.axis_index('pair') * (nq // 2) + lax.axis_index('side')
    cw = w_gate.shape[0] // nq
    return jnp.stack([
        lax.dynamic_slice_in_dim(w_gate, qi * cw, cw, 0),
        lax.dynamic_slice_in_dim(w_up, qi * cw, cw, 0),
        lax.dynamic_slice_in_dim(w_down, qi * cw, cw, 1).T,
    ])


def to_ends(piece, step, zn):
    return lax.ppermute(piece, 'tp', [(step, 0), (zn - 1 - step, zn - 1)])


def plane_step(mine):
    over_y = lax.ppermute(mine, 'side', [(c, c ^ 2) for c in range(4)])
    over_x = lax.ppermute(mine, 'pair', [(p, 1 - p) for p in range(2)])
    over_d = lax.ppermute(mine, ('pair', 'side'), [(p * 4 + s, (1 - p) * 4 + (s + 2) % 4) for p in range(2) for s in range(4)])
    return [mine, over_y, over_x, over_d]


def tie(*values):
    return lax.optimization_barrier(values)


def solution(mesh):
    groups = mesh.shape['side']
    zn = mesh.shape['tp']
    nq = mesh.shape['pair'] * groups
    shift_pairs = [(source_idx, (source_idx + 1) % groups) for source_idx in range(groups)]
    group_axes = ('pair', 'side')
    head_spec = P(none, none, 'tp', none)
    cache_spec = P(group_axes, none, none, none, 'tp', none)
    prompt_spec = P(group_axes, none, none, 'tp', none)
    row_spec = P(group_axes, none, none)
    spec_in = (row_spec, P(group_axes), row_spec, cache_spec, cache_spec, P(group_axes, none), P(), head_spec, P(), head_spec, head_spec, P(none, 'tp', none, none), P(), P(none, none, 'tp'), P(none, none, 'tp'), P(none, 'tp', none))
    spec_out = (row_spec, row_spec, prompt_spec, prompt_spec, cache_spec, cache_spec)

    def device_step(x_prompt, s_len, y_tok, k_cache, v_cache, c_len, attn_gain, w_q, w_dkv, w_uk, w_uv, w_o, mlp_gain, w_gate, w_up, w_down):
        layer = (attn_gain, w_q, w_dkv, w_uk, w_uv, w_o, mlp_gain, w_gate, w_up, w_down)
        attn_gain, w_q, w_dkv, w_uk, w_uv, w_o, mlp_gain, w_gate, w_up, w_down = (v[0] for v in layer)
        zi = lax.axis_index('tp')
        hidden, toks = x_prompt[0], y_tok[0]
        rows, width = hidden.shape
        nb = toks.shape[0]
        hr = rows // 2
        cur_len = c_len[0]
        own = own_piece(w_gate, w_up, w_down, nq)
        near = to_ends(own, 1, zn)

        some = jnp.concatenate([toks, jnp.zeros((16 - nb, width), toks.dtype)], axis=0)
        positions = jnp.concatenate([jnp.arange(rows, dtype=jnp.int32), cur_len, jnp.zeros((16 - nb,), jnp.int32)])
        normed, latent_raw = latent_call(hidden, some, attn_gain[None].astype(jnp.float32), w_dkv.T)
        latent_pack = finish_latent(latent_raw, positions, w_uk.shape[0])
        received = lax.ppermute(latent_pack[:rows], 'side', shift_pairs)
        nope, rank = w_uk.shape[-1], w_uk.shape[0]
        heads, rope = w_q.shape[1], w_q.shape[2] - nope
        latent, rope_key = latent_pack[:, :rank], latent_pack[:, rank:]
        key_all = jnp.einsum('sr,rhn->hsn', latent, w_uk, preferred_element_type=jnp.float32).astype(jnp.bfloat16)
        value = jnp.einsum('sr,rhv->hsv', latent, w_uv, preferred_element_type=jnp.float32).astype(jnp.bfloat16)
        cos, sin = rope_tables(positions, rope)
        rope_two = jnp.concatenate([rope_key[:rows]] * 2, axis=1)
        normed, own, near, later = tie(normed, own, near, received)
        first = plane_step(near)
        middle = to_ends(own, 2, zn)
        far = to_ends(own, 3, zn)
        p_rows, q_tok = attend_call(normed, w_q.transpose(1, 2, 0), key_all, rope_two, value, cos, sin, s_len, rows, w_q.shape[2] ** -0.5)

        rope_new = jnp.broadcast_to(rope_key[rows:rows + nb, None, :], (nb, heads, rope))
        key_new = jnp.concatenate([key_all[:, rows:rows + nb].transpose(1, 0, 2), rope_new], axis=-1)
        value_new = value[:, rows:rows + nb].transpose(1, 0, 2)
        key_new, value_new, q_tok = tie(key_new, value_new, q_tok)
        q_rope = q_tok[:, :nb, nope:nope + rope] + q_tok[:, :nb, nope + rope:]
        query_tok = jnp.concatenate([q_tok[:, :nb, :nope], q_rope], axis=-1).transpose(1, 0, 2)
        key_old, value_old = k_cache[0, 0], v_cache[0, 0]
        slot_hit = (jnp.arange(key_old.shape[1])[None, :] == cur_len[:, None])[:, :, None, None]
        key_layer = jnp.where(slot_hit, key_new[:, None], key_old)
        value_layer = jnp.where(slot_hit, value_new[:, None], value_old)
        tok_val = cache_attention(query_tok, key_layer, value_layer, cur_len).reshape(nb, -1)
        q_rows = jnp.concatenate([tok_val, jnp.zeros((16 - nb, tok_val.shape[1]), tok_val.dtype)], axis=0)

        x_own = lax.dynamic_slice_in_dim(hidden, jnp.where(zi < zn // 2, 0, hr), hr, 0)
        t_own = jnp.concatenate([toks, jnp.zeros((TOK_PAD - nb, width), toks.dtype)], axis=0).astype(jnp.float32)
        h_mid, t_mid, spread, crossed = reduce_call(p_rows, q_rows, x_own, t_own, w_o.reshape(-1, width), first, middle, far, zn)
        pieces = [*first, middle, far, spread, crossed]

        key_in = expand_keys(received, w_uk)
        value_in = expand_values(later, w_uv)

        h_out, t_out = mlp_call(h_mid, t_mid, mlp_gain[None].astype(jnp.float32), w_gate, w_up, w_down, pieces, zn)
        y_out = t_out[:nb].astype(jnp.bfloat16)
        return (h_out[None], y_out[None], key_in[None, None], value_in[None, None], key_layer[None, None], value_layer[None, None])

    return jax.shard_map(device_step, mesh=mesh, in_specs=spec_in, out_specs=spec_out, check_vma=False)
```
